256 devices in a mesh: seq: 64 (over z, y, core), head: 4 (over x).
Axes of the slice: x: 4, y: 4, z: 8, core: 2. Of those that a mesh axis runs over, the one named last changes fastest.
Arguments:
- query_rows: bfloat16 [32768, 4096], P('seq', 'head'), may hold values from -6 to 6
- key_rows: bfloat16 [32768, 4096], P('seq', 'head'), may hold values from -2 to 2
- value_rows: bfloat16 [32768, 4096], P('seq', 'head'), may hold values from -6 to 6
- key_gain: float32 [32], P('head'), may hold values from 0.9 to 1.85, as said below
- regularizer: float32 [32], P('head'), may hold values from 0.5 to 4
Outputs:
- readout: bfloat16 [32768, 4096], P('seq', 'head')
The draws below stay inside these ranges and needn't reach their ends.
Inputs may be any that keep to these rules, and one draw needn't show every extreme that they name: `key_gain`: one positive gain for each head.
All inputs are finite; a program needn't handle non-finite values.
Results may differ from the reference program's by a relative error of at most 0.006.
Values sent between devices are 32-bit elements; how exact they have to be, the bound alone decides.
No kernel may reach another device: no remote copies, remote signals or barrier semaphores. Data moves between devices by JAX's collectives and lax.ppermute only.
A program may use at most 192 MiB of HBM per device.

```python
import math
import jax
import jax.numpy as jnp
from jax import lax

DH = 128
HEADS = 32
TOK_DEV = 512
NS_STEPS = 8
REFINE = 2
SEQ = 32768


def draw_key_gain(key, part):
    position = jnp.arange(HEADS, dtype=jnp.float32) / (HEADS - 1)
    return jnp.exp(0.5 * position + jax.random.uniform(key, (HEADS,), jnp.float32, -0.1, 0.1))


def draw_key_rows(key, part):
    column_key = jax.random.fold_in(key, 11)
    entry_key = jax.random.fold_in(key, 12)
    width = HEADS * DH
    amplitude = jnp.exp(jax.random.uniform(column_key, (width,), jnp.float32, math.log(0.3), math.log(2.4)))
    entries = jax.random.truncated_normal(entry_key, -4.0, 4.0, (SEQ, width), jnp.float32)
    return (entries * amplitude[None, :] / math.sqrt(DH)).astype(jnp.bfloat16)


def steps_of(key, dims, shards, low, largest):
    level = 1.0
    for axis_at, blocks in shards:
        heights = jax.random.uniform(jax.random.fold_in(jax.random.fold_in(key, 6), axis_at), (blocks,), jnp.float32, low / len(shards), largest / len(shards))
        level = level * jnp.repeat(jnp.exp(heights), dims[axis_at] // blocks).reshape((-1,) + (1,) * (len(dims) - 1 - axis_at))
    return level


def gaussian(stream_key, extent, scale, most, cuts=(), held_as=jnp.bfloat16):
    gain = steps_of(stream_key, extent, cuts, -0.22, 0.18) if cuts else 1.0
    values = jax.random.normal(stream_key, extent, jnp.float32) * scale * gain
    return jnp.minimum(jnp.maximum(values, -most), most).astype(held_as)


def setup_inputs(seed: int = 0) -> dict:
    seeds = jax.random.split(jax.random.key(seed), 6)
    return {
        "query_rows": gaussian(seeds[0], (SEQ, HEADS * DH), 1.0, 6.0, ((0, 64), (1, 4))),
        "key_rows": draw_key_rows(jax.random.fold_in(seeds[5], 71), 0),
        "value_rows": gaussian(seeds[2], (SEQ, HEADS * DH), 1.0, 6.0, ((0, 64), (1, 4))),
        "key_gain": draw_key_gain(jax.random.fold_in(seeds[5], 71), 0),
        "regularizer": jnp.clip(jnp.exp(math.log(4.0) - 2.0794415 * jax.random.uniform(seeds[4], (HEADS,), jnp.float32) ** steps_of(seeds[4], (HEADS,), ((0, 4),), -0.2, 0.2)), 0.5, 4.0),
    }


highest = lax.Precision.HIGHEST

def contract_rows(left, right):
    return lax.dot_general(left, right, (((1,), (1,)), ((), ())), preferred_element_type=jnp.float32)

def invert_scaled(end_matrix, spectral_bound):
    identity = jnp.eye(end_matrix.shape[-1], dtype=jnp.float32)
    approx = identity[None, :, :] / spectral_bound[:, None, None]
    for iteration in range(NS_STEPS):
        product = jnp.einsum('hij,hjk->hik', end_matrix, approx, precision=highest)
        approx = jnp.einsum('hij,hjk->hik', approx, 2.0 * identity - product, precision=highest)
    return approx

def solve_head(operands):
    query_head, key_head, value_head, base_matrix, precond, cross_matrix = operands
    length = query_head.shape[0]
    causal = jnp.arange(length)[:, None] >= jnp.arange(length)[None, :]
    query_float = query_head.astype(jnp.float32)
    solution = jnp.dot(query_float, precond, precision=highest)
    for repeat in range(REFINE):
        scores = jnp.where(causal, contract_rows(solution.astype(jnp.bfloat16), key_head), 0.0).astype(jnp.bfloat16)
        in_block = jnp.dot(scores, key_head, preferred_element_type=jnp.float32)
        residual = query_float - jnp.dot(solution, base_matrix, precision=highest) - in_block
        solution = solution + jnp.dot(residual, precond, precision=highest)
    scores = jnp.where(causal, contract_rows(solution.astype(jnp.bfloat16), key_head), 0.0).astype(jnp.bfloat16)
    total = jnp.dot(solution, cross_matrix, precision=highest) + jnp.dot(scores, value_head, preferred_element_type=jnp.float32)
    return total.astype(jnp.bfloat16)

def reference(query_rows, key_rows, value_rows, key_gain, regularizer):
    block_count = query_rows.shape[0] // TOK_DEV
    split_shape = (block_count, TOK_DEV, HEADS, DH)
    identity = jnp.eye(DH, dtype=jnp.float32)

    def block_step(carry, operands):
        prior_gram, prior_cross = carry
        query_block, key_block, value_block = operands
        scaled = (key_block.astype(jnp.float32) * key_gain[None, :, None]).astype(jnp.bfloat16)
        scaled_float = scaled.astype(jnp.float32)
        gram_block = jnp.einsum('thd,the->hde', scaled_float, scaled_float, precision=highest)
        cross_block = jnp.einsum('thd,the->hde', scaled_float, value_block.astype(jnp.float32), precision=highest)
        base_matrix = regularizer[:, None, None] * identity + prior_gram
        end_matrix = base_matrix + gram_block
        spectral_bound = jnp.sqrt(lax.optimization_barrier(jnp.sum(end_matrix * end_matrix, axis=(1, 2))))
        precond = invert_scaled(end_matrix, spectral_bound)
        readout = lax.map(solve_head, (jnp.transpose(query_block, (1, 0, 2)), jnp.transpose(scaled, (1, 0, 2)), jnp.transpose(value_block, (1, 0, 2)), base_matrix, precond, prior_cross))
        merged = jnp.transpose(readout, (1, 0, 2)).reshape(TOK_DEV, HEADS * DH)
        return ((prior_gram + gram_block, prior_cross + cross_block), merged)
    empty_state = jnp.zeros((HEADS, DH, DH), jnp.float32)
    final_carry, outputs = lax.scan(block_step, (empty_state, empty_state), (query_rows.reshape(split_shape), key_rows.reshape(split_shape), value_rows.reshape(split_shape)))
    return outputs.reshape(block_count * TOK_DEV, HEADS * DH)
```

```python
import functools
import jax
import jax.numpy as jnp
from jax import lax
from jax.experimental import pallas as pl
from jax.experimental.pallas import tpu as pltpu
from jax.sharding import Mesh
from jax.sharding import PartitionSpec as P

DH = 128
NS_STEPS = 8
REFINE = 2
CHUNK = 256
VMEM = 16 * 2**20
SEQ = ("seq_0", "seq_1", "seq_2")
PLANE = ("seq_0", "seq_1")
CORE = "seq_2"

f32 = jnp.float32
bf16 = jnp.bfloat16


def mm(left, right):
    return jnp.dot(left, right, preferred_element_type=f32)


def mm_tn(left, right):
    return lax.dot_general(left, right, (((0,), (0,)), ((), ())), preferred_element_type=f32)


def mm_nt(left, right):
    return lax.dot_general(left, right, (((1,), (1,)), ((), ())), preferred_element_type=f32)


def split(x):
    high = x.astype(bf16)
    return high, (x - high.astype(f32)).astype(bf16)


def side(x):
    return jnp.concatenate(split(x), axis=1)


def doubled(x):
    x = side(x)
    return jnp.concatenate([x, x], axis=0)


def fold(x):
    return x[:, :DH] + x[:, DH:]


def eye():
    rows = lax.broadcasted_iota(jnp.int32, (DH, DH), 0)
    columns = lax.broadcasted_iota(jnp.int32, (DH, DH), 1)
    return (rows == columns).astype(f32)


def scaled_keys(key, gain):
    return (key.astype(f32) * gain).astype(bf16)


def gram_kernel(core_ref, gain_ref, k0_ref, v0_ref, k1_ref, v1_ref, keep_ref, send_ref):
    i = pl.program_id(0)
    core = core_ref[0]
    for k_ref, v_ref, out_ref, half in ((k0_ref, v0_ref, keep_ref, core), (k1_ref, v1_ref, send_ref, 1 - core)):
        k = scaled_keys(k_ref[...], gain_ref[half * pl.num_programs(0) + i])
        both = mm_tn(k, jnp.concatenate([k, v_ref[...]], axis=1))
        out_ref[0, 0] = both[:, :DH]
        out_ref[0, 1] = both[:, DH:]


def grams(core, gain, key, value):
    rows, width = key.shape
    half = width // DH // 2
    mine = pl.BlockSpec((rows, DH), lambda i, c: (0, i + half * c[0]))
    other = pl.BlockSpec((rows, DH), lambda i, c: (0, i + half * (1 - c[0])))
    out = pl.BlockSpec((1, 2, DH, DH), lambda i, c: (i, 0, 0, 0))
    shape = jax.ShapeDtypeStruct((half, 2, DH, DH), f32)
    return pl.pallas_call(
        gram_kernel,
        grid_spec=pltpu.PrefetchScalarGridSpec(
            num_scalar_prefetch=1,
            grid=(half,),
            in_specs=[pl.BlockSpec(memory_space=pltpu.SMEM), mine, mine, other, other],
            out_specs=[out, out],
        ),
        out_shape=[shape, shape],
        compiler_params=pltpu.CompilerParams(vmem_limit_bytes=VMEM),
        name="grams",
    )(core, gain, key, value, key, value)


def first_kernel(core_ref, gain_ref, k_ref, v_ref, gram_ref, cross_ref):
    heads = 2 * pl.num_programs(0)
    for a in range(2):
        h = lax.rem(2 * pl.program_id(0) + a + core_ref[0] * (heads // 2), heads)
        columns = slice(a * DH, (a + 1) * DH)
        k = scaled_keys(k_ref[:, columns], gain_ref[h])
        both = mm_tn(k, jnp.concatenate([k, v_ref[:, columns]], axis=1))
        gram_ref[a] = both[:, :DH]
        cross_ref[a] = both[:, DH:]


def first_grams(core, gain, key, value):
    steps = key.shape[1] // DH // 2
    block = pl.BlockSpec((CHUNK, 2 * DH), lambda i, c: (0, lax.rem(i + c[0] * (steps // 2), steps)))
    out = pl.BlockSpec((2, DH, DH), lambda i, c: (i, 0, 0))
    shape = jax.ShapeDtypeStruct((2 * steps, DH, DH), f32)
    return pl.pallas_call(
        first_kernel,
        grid_spec=pltpu.PrefetchScalarGridSpec(
            num_scalar_prefetch=1,
            grid=(steps,),
            in_specs=[pl.BlockSpec(memory_space=pltpu.SMEM), block, block],
            out_specs=[out, out],
        ),
        out_shape=[shape, shape],
        cost_estimate=pl.CostEstimate(flops=2 * 10**9, bytes_accessed=2 * 10**6, transcendentals=0),
        compiler_params=pltpu.CompilerParams(vmem_limit_bytes=VMEM),
        name="first_grams",
    )(core, gain, key, value)


def running_kernel(x_ref, o_ref):
    total = x_ref[0]
    o_ref[0] = jnp.zeros_like(total)
    for j in range(1, x_ref.shape[0]):
        o_ref[j] = total
        if j < x_ref.shape[0] - 1:
            total = total + x_ref[j]


def sums_before(pieces):
    return pl.pallas_call(
        running_kernel,
        out_shape=jax.ShapeDtypeStruct(pieces.shape, f32),
        in_specs=[pl.BlockSpec(memory_space=pltpu.VMEM)],
        out_specs=pl.BlockSpec(memory_space=pltpu.VMEM),
        compiler_params=pltpu.CompilerParams(vmem_limit_bytes=VMEM),
        name="sums_before",
    )(pieces)


def precond_kernel(core_ref, reg_ref, mine_ref, other_ref, keep_ref, send_ref, base_ref, y_ref):
    identity = eye()
    half = mine_ref.shape[0]
    inverse, approx, product = [], [], []
    for i in range(2 * half):
        first = i < half
        prior_ref, block_ref = (mine_ref, keep_ref) if first else (other_ref, send_ref)
        h = (core_ref[0] if first else 1 - core_ref[0]) * half + i % half
        base = identity * reg_ref[h] + prior_ref[i % half, 0]
        base_ref[i] = base
        end = base + block_ref[i % half, 0]
        squares = jnp.sum(jnp.sum(end * end, axis=0, keepdims=True), axis=1, keepdims=True)
        inv = 1.0 / jnp.sqrt(squares)
        z = end * inv
        inverse.append(inv)
        approx.append(2.0 * identity - z)
        product.append(2.0 * z - fold(mm(side(z), doubled(z))))
    for step in range(NS_STEPS - 2):
        for i in range(2 * half):
            both = jnp.concatenate([approx[i], product[i]], axis=0)
            both = 2.0 * both - fold(mm(side(both), doubled(product[i])))
            approx[i], product[i] = both[:DH], both[DH:]
    for i in range(2 * half):
        last = 2.0 * approx[i] - fold(mm(side(approx[i]), doubled(product[i])))
        y_ref[i] = last * inverse[i]


def preconditioners(core, reg, mine, other, keep, send):
    half = mine.shape[0]
    smem = pl.BlockSpec(memory_space=pltpu.SMEM)
    matrices = pl.BlockSpec((half, 1, DH, DH), lambda i: (0, 0, 0, 0))
    out = pl.BlockSpec((2 * half, DH, DH), lambda i: (0, 0, 0))
    shape = jax.ShapeDtypeStruct((2 * half, DH, DH), f32)
    return pl.pallas_call(
        precond_kernel,
        grid=(1,),
        in_specs=[smem, smem] + [matrices] * 4,
        out_specs=[out, out],
        out_shape=[shape, shape],
        compiler_params=pltpu.CompilerParams(vmem_limit_bytes=VMEM),
        name="preconditioners",
    )(core, reg, mine, other, keep, send)


def solve_kernel(core_ref, gain_ref, q_ref, k_ref, v_ref, y_ref, base_ref, gram_ref, mine_ref, other_ref, cross_ref, o_ref):
    step = pl.program_id(0)
    heads = 2 * pl.num_programs(0)
    shape = (CHUNK, CHUNK)
    causal = lax.broadcasted_iota(jnp.int32, shape, 0) >= lax.broadcasted_iota(jnp.int32, shape, 1)
    chains = []
    for a in range(2):
        h = lax.rem(2 * step + a + core_ref[0] * (heads // 2), heads)
        columns = slice(a * DH, (a + 1) * DH)
        k = scaled_keys(k_ref[:, columns], gain_ref[h])
        y = side(y_ref[a])
        cross = jnp.where(step < heads // 4, mine_ref[a, 0], other_ref[a, 0])
        for j in range(k.shape[0] // CHUNK):
            rows = slice(j * CHUNK, (j + 1) * CHUNK)
            base, prior = base_ref[a], cross
            if j:
                base, prior = base + gram_ref[a], prior + cross_ref[a]
            chains.append(
                dict(
                    at=(rows, columns), q=q_ref[rows, columns], k=k[rows], v=v_ref[rows, columns], y=y,
                    yy=jnp.concatenate([y, y], axis=0), base=doubled(base), prior=doubled(prior),
                )
            )
    for c in chains:
        c["s"] = fold(mm(c["q"], c["y"]))
    for repeat in range(REFINE):
        for c in chains:
            c["parts"] = split(c["s"])
            c["scores"] = jnp.where(causal, mm_nt(c["parts"][0], c["k"]), 0.0).astype(bf16)
        for c in chains:
            product = fold(mm(jnp.concatenate(c["parts"], axis=1), c["base"]))
            c["residual"] = c["q"].astype(f32) - product - mm(c["scores"], c["k"])
        for c in chains:
            c["s"] = c["s"] + fold(mm(side(c["residual"]), c["yy"]))
    for c in chains:
        parts = split(c["s"])
        scores = jnp.where(causal, mm_nt(parts[0], c["k"]), 0.0).astype(bf16)
        total = fold(mm(jnp.concatenate(parts, axis=1), c["prior"])) + mm(scores, c["v"])
        o_ref[c["at"]] = total.astype(bf16)


def solve(core, gain, query, key, value, y, base, gram, mine, other, cross):
    rows, width = query.shape
    steps = width // DH // 2
    smem = pl.BlockSpec(memory_space=pltpu.SMEM)
    wide = pl.BlockSpec((rows, 2 * DH), lambda i, c: (0, lax.rem(i + c[0] * (steps // 2), steps)))
    matrices = pl.BlockSpec((2, DH, DH), lambda i, c: (i, 0, 0))
    low = pl.BlockSpec((2, 1, DH, DH), lambda i, c: (jnp.minimum(i, steps // 2 - 1), 1, 0, 0))
    high = pl.BlockSpec((2, 1, DH, DH), lambda i, c: (jnp.maximum(i - steps // 2, 0), 1, 0, 0))
    return pl.pallas_call(
        solve_kernel,
        grid_spec=pltpu.PrefetchScalarGridSpec(
            num_scalar_prefetch=1,
            grid=(steps,),
            in_specs=[smem, wide, wide, wide, matrices, matrices, matrices, low, high, matrices],
            out_specs=wide,
        ),
        out_shape=jax.ShapeDtypeStruct((rows, width), bf16),
        compiler_params=pltpu.CompilerParams(vmem_limit_bytes=VMEM),
        name="solve",
    )(core, gain, query, key, value, y, base, gram, mine, other, cross)


def body(query_rows, key_rows, value_rows, key_gain, regularizer):
    place = lax.axis_index(CORE)
    core = place.astype(jnp.int32).reshape(1)
    swap = [(0, 1), (1, 0)]
    chips = lax.axis_size(PLANE)
    keep, send = grams(core, key_gain, key_rows, value_rows)
    received = lax.ppermute(send, CORE, swap)
    pieces = (keep + received).reshape(chips, -1, DH)
    pieces = lax.all_to_all(pieces, PLANE, 0, 0)
    first_gram, first_cross = first_grams(core, key_gain, key_rows, value_rows)
    before = lax.all_to_all(sums_before(pieces), PLANE, 0, 0).reshape(keep.shape)
    mine = before + jnp.where(place == 1, received, 0.0)
    other = lax.ppermute(before + jnp.where(place == 0, keep, 0.0), CORE, swap)
    base, y = preconditioners(core, regularizer, mine, other, keep, send)
    return solve(
        core, key_gain, query_rows, key_rows, value_rows, y, base, first_gram, mine, other, first_cross
    )


def solution(mesh):
    torus = Mesh(
        mesh.devices.reshape(8, 4, 2, mesh.shape["head"]), ("seq_0", "seq_1", "seq_2", "head")
    )
    in_specs = (P(SEQ, "head"), P(SEQ, "head"), P(SEQ, "head"), P("head"), P("head"))
    out_specs = P(SEQ, "head")
    return jax.shard_map(body, mesh=torus, in_specs=in_specs, out_specs=out_specs, check_vma=False)
```

```python
import functools
import jax
import jax.numpy as jnp
from jax import lax
from jax.experimental import pallas as pl
from jax.experimental.pallas import tpu as pltpu
from jax.sharding import Mesh
from jax.sharding import PartitionSpec as P

DH = 128
NS_STEPS = 8
REFINE = 2
CHUNK = 256
VMEM = 16 * 2**20
SEQ = ("seq_0", "seq_1", "seq_2")
PLANE = ("seq_0", "seq_1")
CORE = "seq_2"

f32 = jnp.float32
bf16 = jnp.bfloat16


def mm(left, right):
    return jnp.dot(left, right, preferred_element_type=f32)


def mm_tn(left, right):
    return lax.dot_general(left, right, (((0,), (0,)), ((), ())), preferred_element_type=f32)


def mm_nt(left, right):
    return lax.dot_general(left, right, (((1,), (1,)), ((), ())), preferred_element_type=f32)


def split(x):
    high = x.astype(bf16)
    return high, (x - high.astype(f32)).astype(bf16)


def side(x):
    return jnp.concatenate(split(x), axis=1)


def doubled(x):
    x = side(x)
    return jnp.concatenate([x, x], axis=0)


def fold(x):
    return x[:, :DH] + x[:, DH:]


def eye():
    rows = lax.broadcasted_iota(jnp.int32, (DH, DH), 0)
    columns = lax.broadcasted_iota(jnp.int32, (DH, DH), 1)
    return (rows == columns).astype(f32)


def scaled_keys(key, gain):
    return (key.astype(f32) * gain).astype(bf16)


def in_hbm(*arrays):
    return [pltpu.with_memory_space_constraint(x, pltpu.HBM) for x in arrays]


def place_of(core_ref, step, heads):
    return lax.rem(step + core_ref[0] * (heads // 2), heads)


def gram_kernel(core_ref, gain_ref, reg_ref, k_ref, v_ref, keep_ref, send_ref, first_ref, scaled_ref, ridge_ref):
    step = pl.program_id(0)
    heads = 2 * pl.num_programs(0)
    both = []
    for a in range(2):
        h = place_of(core_ref, 2 * step + a, heads)
        columns = slice(a * DH, (a + 1) * DH)
        k = scaled_keys(k_ref[:, columns], gain_ref[h])
        scaled_ref[:, columns] = k
        ridge_ref[a] = jnp.full(ridge_ref.shape[1:], reg_ref[h])
        pair = jnp.concatenate([k, v_ref[:, columns]], axis=1)
        first = mm_tn(k[:CHUNK], pair[:CHUNK])
        first_ref[a, 0] = first[:, :DH]
        first_ref[a, 1] = first[:, DH:]
        both.append(first + mm_tn(k[CHUNK:], pair[CHUNK:]))

    def put(out_ref):
        for a in range(2):
            out_ref[a, 0] = both[a][:, :DH]
            out_ref[a, 1] = both[a][:, DH:]

    @pl.when(step < heads // 4)
    def _():
        put(keep_ref)

    @pl.when(step >= heads // 4)
    def _():
        put(send_ref)


def grams(core, gain, reg, key, value):
    gain, reg, key, value = in_hbm(gain, reg, key, value)
    rows, width = key.shape
    heads = width // DH
    steps = heads // 2
    smem = pl.BlockSpec(memory_space=pltpu.SMEM)
    wide = pl.BlockSpec((rows, 2 * DH), lambda i, c: (0, lax.rem(i + c[0] * (steps // 2), steps)))
    low = pl.BlockSpec((2, 2, DH, DH), lambda i, c: (jnp.minimum(i, steps // 2 - 1), 0, 0, 0))
    high = pl.BlockSpec((2, 2, DH, DH), lambda i, c: (jnp.maximum(i - steps // 2, 0), 0, 0, 0))
    every = pl.BlockSpec((2, 2, DH, DH), lambda i, c: (i, 0, 0, 0))
    half = jax.ShapeDtypeStruct((heads // 2, 2, DH, DH), f32)
    return pl.pallas_call(
        gram_kernel,
        grid_spec=pltpu.PrefetchScalarGridSpec(
            num_scalar_prefetch=1,
            grid=(steps,),
            in_specs=[smem, smem, wide, wide],
            out_specs=[low, high, every, wide, pl.BlockSpec((2, 8, DH), lambda i, c: (i, 0, 0))],
        ),
        out_shape=[
            half,
            half,
            jax.ShapeDtypeStruct((heads, 2, DH, DH), f32),
            jax.ShapeDtypeStruct((rows, width), bf16),
            jax.ShapeDtypeStruct((heads, 8, DH), f32),
        ],
        compiler_params=pltpu.CompilerParams(vmem_limit_bytes=VMEM),
        name="grams",
    )(core, gain, reg, key, value)


def running_kernel(x_ref, o_ref):
    total = x_ref[0]
    o_ref[0] = jnp.zeros_like(total)
    for j in range(1, x_ref.shape[0]):
        o_ref[j] = total
        if j < x_ref.shape[0] - 1:
            total = total + x_ref[j]


def sums_before(pieces):
    return pl.pallas_call(
        running_kernel,
        out_shape=jax.ShapeDtypeStruct(pieces.shape, f32),
        in_specs=[pl.BlockSpec(memory_space=pltpu.VMEM)],
        out_specs=pl.BlockSpec(memory_space=pltpu.VMEM),
        compiler_params=pltpu.CompilerParams(vmem_limit_bytes=VMEM),
        name="sums_before",
    )(pieces)


def precond_kernel(ridge_ref, prior_ref, block_ref, base_ref, y_ref):
    identity = eye()
    heads = range(prior_ref.shape[0])
    inverse, approx, product = [], [], []
    for i in heads:
        base = identity * ridge_ref[i, :1] + prior_ref[i, 0]
        base_ref[i] = base
        end = base + block_ref[i, 0]
        squares = jnp.sum(jnp.sum(end * end, axis=0, keepdims=True), axis=1, keepdims=True)
        inv = 1.0 / jnp.sqrt(squares)
        z = end * inv
        inverse.append(inv)
        approx.append(2.0 * identity - z)
        product.append(2.0 * z - fold(mm(side(z), doubled(z))))
    for step in range(NS_STEPS - 2):
        for i in heads:
            both = jnp.concatenate([approx[i], product[i]], axis=0)
            both = 2.0 * both - fold(mm(side(both), doubled(product[i])))
            approx[i], product[i] = both[:DH], both[DH:]
    for i in heads:
        last = 2.0 * approx[i] - fold(mm(side(approx[i]), doubled(product[i])))
        y_ref[i] = last * inverse[i]


def preconditioners(ridge, at, prior, block):
    half = prior.shape[0]
    matrices = pl.BlockSpec((half, 2, DH, DH), lambda i: (0, 0, 0, 0))
    out = pl.BlockSpec((half, DH, DH), lambda i: (0, 0, 0))
    shape = jax.ShapeDtypeStruct((half, DH, DH), f32)
    return pl.pallas_call(
        precond_kernel,
        grid=(1,),
        in_specs=[pl.BlockSpec((half, 8, DH), lambda i: (at, 0, 0)), matrices, matrices],
        out_specs=[out, out],
        out_shape=[shape, shape],
        compiler_params=pltpu.CompilerParams(vmem_limit_bytes=VMEM),
        cost_estimate=pl.CostEstimate(flops=10**9, bytes_accessed=2 * 10**6, transcendentals=0),
        name="preconditioners",
    )(ridge, prior, block)


def solve_kernel(core_ref, q_ref, k_ref, v_ref, first_ref, *refs):
    half_refs, o_ref = refs[:6], refs[6]
    low = pl.program_id(0) < pl.num_programs(0) // 2
    shape = (CHUNK, CHUNK)
    causal = lax.broadcasted_iota(jnp.int32, shape, 0) >= lax.broadcasted_iota(jnp.int32, shape, 1)
    chains = []
    for a in range(2):
        columns = slice(a * DH, (a + 1) * DH)
        y0, base, cross = [
            jnp.where(low, half_refs[n][a], half_refs[n + 1][a])
            if n < 4
            else jnp.where(low, half_refs[n][a, 0], half_refs[n + 1][a, 0])
            for n in (0, 2, 4)
        ]
        y = side(y0)
        for j in range(k_ref.shape[0] // CHUNK):
            rows = slice(j * CHUNK, (j + 1) * CHUNK)
            if j:
                base, cross = base + first_ref[a, 0], cross + first_ref[a, 1]
            chains.append(
                dict(
                    at=(rows, columns), q=q_ref[rows, columns], k=k_ref[rows, columns],
                    v=v_ref[rows, columns], y=y, yy=jnp.concatenate([y, y], axis=0),
                    base=doubled(base), prior=doubled(cross),
                )
            )
    for c in chains:
        c["s"] = fold(mm(c["q"], c["y"]))
    for repeat in range(REFINE):
        for c in chains:
            c["parts"] = split(c["s"])
            c["scores"] = jnp.where(causal, mm_nt(c["parts"][0], c["k"]), 0.0).astype(bf16)
        for c in chains:
            product = fold(mm(jnp.concatenate(c["parts"], axis=1), c["base"]))
            c["residual"] = c["q"].astype(f32) - product - mm(c["scores"], c["k"])
        for c in chains:
            c["s"] = c["s"] + fold(mm(side(c["residual"]), c["yy"]))
    for c in chains:
        parts = split(c["s"])
        scores = jnp.where(causal, mm_nt(parts[0], c["k"]), 0.0).astype(bf16)
        total = fold(mm(jnp.concatenate(parts, axis=1), c["prior"])) + mm(scores, c["v"])
        o_ref[c["at"]] = total.astype(bf16)


def solve(core, query, key, value, first, halves):
    rows, width = query.shape
    steps = width // DH // 2
    at_low = lambda i: jnp.minimum(i, steps // 2 - 1)
    at_high = lambda i: jnp.maximum(i - steps // 2, 0)
    wide = pl.BlockSpec((rows, 2 * DH), lambda i, c: (0, lax.rem(i + c[0] * (steps // 2), steps)))
    specs = []
    for at in (at_low, at_high) * 2:
        specs.append(pl.BlockSpec((2, DH, DH), lambda i, c, at=at: (at(i), 0, 0)))
    for at in (at_low, at_high):
        specs.append(pl.BlockSpec((2, 1, DH, DH), lambda i, c, at=at: (at(i), 1, 0, 0)))
    return pl.pallas_call(
        solve_kernel,
        grid_spec=pltpu.PrefetchScalarGridSpec(
            num_scalar_prefetch=1,
            grid=(steps,),
            in_specs=[wide, wide, wide, pl.BlockSpec((2, 2, DH, DH), lambda i, c: (i, 0, 0, 0))] + specs,
            out_specs=wide,
        ),
        out_shape=jax.ShapeDtypeStruct((rows, width), bf16),
        compiler_params=pltpu.CompilerParams(vmem_limit_bytes=VMEM),
        name="solve",
    )(core, query, key, value, first, *halves)


def exchange(x):
    return lax.all_to_all(x, PLANE, 0, 0)


def swapped(x):
    return lax.ppermute(x, CORE, [(0, 1), (1, 0)])


def body(query_rows, key_rows, value_rows, key_gain, regularizer):
    place = lax.axis_index(CORE)
    core = place.astype(jnp.int32).reshape(1)
    chips = lax.axis_size(PLANE)
    core, is_first, is_second = lax.optimization_barrier((core, place == 0, place == 1))
    keep, send, first, scaled, ridge = grams(core, key_gain, regularizer, key_rows, value_rows)
    received = swapped(send)
    pieces = exchange((keep + received).reshape(chips, -1, DH))
    before = exchange(sums_before(pieces)).reshape(keep.shape)
    mine = before + jnp.where(is_second, received, 0.0)
    other = swapped(before + jnp.where(is_first, keep, 0.0))
    base0, y0 = preconditioners(ridge, 0, mine, keep)
    base1, y1 = preconditioners(ridge, 1, other, send)
    return solve(
        core, query_rows, scaled, value_rows, first, (y0, y1, base0, base1, mine, other)
    )


def solution(mesh):
    torus = Mesh(
        mesh.devices.reshape(8, 4, 2, mesh.shape["head"]), ("seq_0", "seq_1", "seq_2", "head")
    )
    in_specs = (P(SEQ, "head"), P(SEQ, "head"), P(SEQ, "head"), P("head"), P("head"))
    out_specs = P(SEQ, "head")
    return jax.shard_map(body, mesh=torus, in_specs=in_specs, out_specs=out_specs, check_vma=False)
```

```python
import functools
import jax
import jax.numpy as jnp
from jax import lax
from jax.experimental import pallas as pl
from jax.experimental.pallas import tpu as pltpu
from jax.sharding import Mesh
from jax.sharding import PartitionSpec as P

DH = 128
NS_STEPS = 8
REFINE = 2
CHUNK = 256
VMEM = 16 * 2**20
PAIR = 400
SEQ = ("seq_0", "seq_1", "seq_2")
PLANE = ("seq_0", "seq_1")
CORE = "seq_2"

f32 = jnp.float32
bf16 = jnp.bfloat16


def mm(left, right):
    return jnp.dot(left, right, preferred_element_type=f32)


def mm_tn(left, right):
    return lax.dot_general(left, right, (((0,), (0,)), ((), ())), preferred_element_type=f32)


def mm_nt(left, right):
    return lax.dot_general(left, right, (((1,), (1,)), ((), ())), preferred_element_type=f32)


def split(x):
    high = x.astype(bf16)
    return high, (x - high.astype(f32)).astype(bf16)


def side(x):
    return jnp.concatenate(split(x), axis=1)


def doubled(x):
    x = side(x)
    return jnp.concatenate([x, x], axis=0)


def fold(x):
    return x[:, :DH] + x[:, DH:]


def eye():
    rows = lax.broadcasted_iota(jnp.int32, (DH, DH), 0)
    columns = lax.broadcasted_iota(jnp.int32, (DH, DH), 1)
    return (rows == columns).astype(f32)


def scaled_keys(key, gain):
    return (key.astype(f32) * gain).astype(bf16)


def in_hbm(*arrays):
    return [pltpu.with_memory_space_constraint(x, pltpu.HBM) for x in arrays]


def place_of(core_ref, step, heads):
    return lax.rem(step + core_ref[0] * (heads // 2), heads)


def triangles():
    rows = lax.broadcasted_iota(jnp.int32, (DH, DH), 0)
    columns = lax.broadcasted_iota(jnp.int32, (DH, DH), 1)
    return rows <= columns, rows == columns


def gram_kernel(core_ref, gain_ref, reg_ref, k_ref, v_ref, keep_ref, send_ref, local_ref, scaled_ref, ridge_ref):
    step = pl.program_id(0)
    heads = 2 * pl.num_programs(0)
    both = []
    for a in range(2):
        h = place_of(core_ref, 2 * step + a, heads)
        columns = slice(a * DH, (a + 1) * DH)
        k = scaled_keys(k_ref[:, columns], gain_ref[h])
        scaled_ref[:, columns] = k
        ridge_ref[a] = jnp.full(ridge_ref.shape[1:], reg_ref[h])
        pair = jnp.concatenate([k, v_ref[:, columns]], axis=1)
        first = mm_tn(k[:CHUNK], pair[:CHUNK])
        local_ref[a, 0] = first[:, :DH]
        local_ref[a, 1] = first[:, DH:]
        both.append(first + mm_tn(k[CHUNK:], pair[CHUNK:]))
        local_ref[a, 2] = both[a][:, :DH]
    one, two = both[0][:, :DH], both[1][:, :DH]
    above, on = triangles()
    packed = jnp.where(above, one, two)
    diagonal = jnp.sum(jnp.where(on, two, 0.0), axis=0, keepdims=True)

    def put(out_ref):
        for a in range(2):
            out_ref[0, a * DH : (a + 1) * DH] = both[a][:, DH:]
        out_ref[0, 2 * DH : 3 * DH] = packed
        out_ref[0, 3 * DH :] = jnp.broadcast_to(diagonal, (PAIR - 3 * DH, DH))

    @pl.when(step < heads // 4)
    def _():
        put(keep_ref)

    @pl.when(step >= heads // 4)
    def _():
        put(send_ref)


def grams(core, gain, reg, key, value):
    gain, reg, key, value = in_hbm(gain, reg, key, value)
    rows, width = key.shape
    heads = width // DH
    steps = heads // 2
    smem = pl.BlockSpec(memory_space=pltpu.SMEM)
    wide = pl.BlockSpec((rows, 2 * DH), lambda i, c: (0, lax.rem(i + c[0] * (steps // 2), steps)))
    low = pl.BlockSpec((1, PAIR, DH), lambda i, c: (jnp.minimum(i, steps // 2 - 1), 0, 0))
    high = pl.BlockSpec((1, PAIR, DH), lambda i, c: (jnp.maximum(i - steps // 2, 0), 0, 0))
    slabs = jax.ShapeDtypeStruct((steps // 2, PAIR, DH), f32)
    return pl.pallas_call(
        gram_kernel,
        grid_spec=pltpu.PrefetchScalarGridSpec(
            num_scalar_prefetch=1,
            grid=(steps,),
            in_specs=[smem, smem, wide, wide],
            out_specs=[
                low,
                high,
                pl.BlockSpec((2, 3, DH, DH), lambda i, c: (i, 0, 0, 0)),
                wide,
                pl.BlockSpec((2, 8, DH), lambda i, c: (i, 0, 0)),
            ],
        ),
        out_shape=[
            slabs,
            slabs,
            jax.ShapeDtypeStruct((heads, 3, DH, DH), f32),
            jax.ShapeDtypeStruct((rows, width), bf16),
            jax.ShapeDtypeStruct((heads, 8, DH), f32),
        ],
        compiler_params=pltpu.CompilerParams(vmem_limit_bytes=VMEM),
        name="grams",
    )(core, gain, reg, key, value)


def running_kernel(x_ref, o_ref):
    total = x_ref[0]
    o_ref[0] = jnp.zeros_like(total)
    for j in range(1, x_ref.shape[0]):
        o_ref[j] = total
        if j < x_ref.shape[0] - 1:
            total = total + x_ref[j]


def sums_before(pieces):
    return pl.pallas_call(
        running_kernel,
        out_shape=jax.ShapeDtypeStruct(pieces.shape, f32),
        in_specs=[pl.BlockSpec(memory_space=pltpu.VMEM)],
        out_specs=pl.BlockSpec(memory_space=pltpu.VMEM),
        compiler_params=pltpu.CompilerParams(vmem_limit_bytes=VMEM),
        name="sums_before",
    )(pieces)


def precond_kernel(ridge_ref, prior_ref, local_ref, base_ref, y_ref):
    identity = eye()
    above, on = triangles()
    heads = range(local_ref.shape[0])
    priors = []
    for pair in range(prior_ref.shape[0]):
        packed = prior_ref[pair, 2 * DH : 3 * DH]
        turned = packed.T
        diagonal = prior_ref[pair, 3 * DH : 3 * DH + 1]
        priors.append(jnp.where(above, packed, turned))
        priors.append(jnp.where(on, diagonal, jnp.where(above, turned, packed)))
    inverse, approx, product = [], [], []
    for i in heads:
        base = identity * ridge_ref[i, :1] + priors[i]
        base_ref[i] = base
        end = base + local_ref[i, 0]
        squares = jnp.sum(jnp.sum(end * end, axis=0, keepdims=True), axis=1, keepdims=True)
        inv = 1.0 / jnp.sqrt(squares)
        z = end * inv
        inverse.append(inv)
        approx.append(2.0 * identity - z)
        product.append(2.0 * z - fold(mm(side(z), doubled(z))))
    for step in range(NS_STEPS - 2):
        for i in heads:
            both = jnp.concatenate([approx[i], product[i]], axis=0)
            both = 2.0 * both - fold(mm(side(both), doubled(product[i])))
            approx[i], product[i] = both[:DH], both[DH:]
    for i in heads:
        last = 2.0 * approx[i] - fold(mm(side(approx[i]), doubled(product[i])))
        y_ref[i] = last * inverse[i]


def preconditioners(ridge, at, prior, local):
    half = 2 * prior.shape[0]
    out = pl.BlockSpec((half, DH, DH), lambda i: (0, 0, 0))
    shape = jax.ShapeDtypeStruct((half, DH, DH), f32)
    return pl.pallas_call(
        precond_kernel,
        grid=(1,),
        in_specs=[
            pl.BlockSpec((half, 8, DH), lambda i: (at, 0, 0)),
            pl.BlockSpec(prior.shape, lambda i: (0, 0, 0)),
            pl.BlockSpec((half, 1, DH, DH), lambda i: (at, 2, 0, 0)),
        ],
        out_specs=[out, out],
        out_shape=[shape, shape],
        compiler_params=pltpu.CompilerParams(vmem_limit_bytes=VMEM),
        cost_estimate=pl.CostEstimate(flops=10**9, bytes_accessed=2 * 10**6, transcendentals=0),
        name="preconditioners",
    )(ridge, prior, local)


def solve_kernel(core_ref, q_ref, k_ref, v_ref, local_ref, *refs):
    half_refs, o_ref = refs[:6], refs[6]
    low = pl.program_id(0) < pl.num_programs(0) // 2
    shape = (CHUNK, CHUNK)
    causal = lax.broadcasted_iota(jnp.int32, shape, 0) >= lax.broadcasted_iota(jnp.int32, shape, 1)
    chains = []
    for a in range(2):
        columns = slice(a * DH, (a + 1) * DH)
        y = side(jnp.where(low, half_refs[0][a], half_refs[1][a]))
        base = jnp.where(low, half_refs[2][a], half_refs[3][a])
        cross = jnp.where(low, half_refs[4][0, columns], half_refs[5][0, columns])
        for j in range(k_ref.shape[0] // CHUNK):
            rows = slice(j * CHUNK, (j + 1) * CHUNK)
            if j:
                base, cross = base + local_ref[a, 0], cross + local_ref[a, 1]
            chains.append(
                dict(
                    at=(rows, columns), q=q_ref[rows, columns], k=k_ref[rows, columns],
                    v=v_ref[rows, columns], y=y, yy=jnp.concatenate([y, y], axis=0),
                    base=doubled(base), prior=doubled(cross),
                )
            )
    for c in chains:
        c["s"] = fold(mm(c["q"], c["y"]))
    for repeat in range(REFINE):
        for c in chains:
            c["parts"] = split(c["s"])
            c["scores"] = jnp.where(causal, mm_nt(c["parts"][0], c["k"]), 0.0).astype(bf16)
        for c in chains:
            product = fold(mm(jnp.concatenate(c["parts"], axis=1), c["base"]))
            c["residual"] = c["q"].astype(f32) - product - mm(c["scores"], c["k"])
        for c in chains:
            c["s"] = c["s"] + fold(mm(side(c["residual"]), c["yy"]))
    for c in chains:
        parts = split(c["s"])
        scores = jnp.where(causal, mm_nt(parts[0], c["k"]), 0.0).astype(bf16)
        total = fold(mm(jnp.concatenate(parts, axis=1), c["prior"])) + mm(scores, c["v"])
        o_ref[c["at"]] = total.astype(bf16)


def solve(core, query, key, value, local, halves):
    rows, width = query.shape
    steps = width // DH // 2
    at_low = lambda i: jnp.minimum(i, steps // 2 - 1)
    at_high = lambda i: jnp.maximum(i - steps // 2, 0)
    wide = pl.BlockSpec((rows, 2 * DH), lambda i, c: (0, lax.rem(i + c[0] * (steps // 2), steps)))
    specs = []
    for at in (at_low, at_high) * 2:
        specs.append(pl.BlockSpec((2, DH, DH), lambda i, c, at=at: (at(i), 0, 0)))
    for at in (at_low, at_high):
        specs.append(pl.BlockSpec((1, 2 * DH, DH), lambda i, c, at=at: (at(i), 0, 0)))
    return pl.pallas_call(
        solve_kernel,
        grid_spec=pltpu.PrefetchScalarGridSpec(
            num_scalar_prefetch=1,
            grid=(steps,),
            in_specs=[wide, wide, wide, pl.BlockSpec((2, 2, DH, DH), lambda i, c: (i, 0, 0, 0))] + specs,
            out_specs=wide,
        ),
        out_shape=jax.ShapeDtypeStruct((rows, width), bf16),
        compiler_params=pltpu.CompilerParams(vmem_limit_bytes=VMEM),
        name="solve",
    )(core, query, key, value, local, *halves)


def exchange(x):
    return lax.all_to_all(x, PLANE, 0, 0)


def swapped(x):
    return lax.ppermute(x, CORE, [(0, 1), (1, 0)])


def body(query_rows, key_rows, value_rows, key_gain, regularizer):
    place = lax.axis_index(CORE)
    core = place.astype(jnp.int32).reshape(1)
    chips = lax.axis_size(PLANE)
    core, is_first, is_second = lax.optimization_barrier((core, place == 0, place == 1))
    keep, send, local, scaled, ridge = grams(core, key_gain, regularizer, key_rows, value_rows)
    received = swapped(send)
    pieces = exchange((keep + received).reshape(chips, 1, -1))
    before = exchange(sums_before(pieces)).reshape(keep.shape)
    mine = before + jnp.where(is_second, received, 0.0)
    other = swapped(before + jnp.where(is_first, keep, 0.0))
    base0, y0 = preconditioners(ridge, 0, mine, local)
    base1, y1 = preconditioners(ridge, 1, other, local)
    return solve(
        core, query_rows, scaled, value_rows, local, (y0, y1, base0, base1, mine, other)
    )


def solution(mesh):
    torus = Mesh(
        mesh.devices.reshape(8, 4, 2, mesh.shape["head"]), ("seq_0", "seq_1", "seq_2", "head")
    )
    in_specs = (P(SEQ, "head"), P(SEQ, "head"), P(SEQ, "head"), P("head"), P("head"))
    out_specs = P(SEQ, "head")
    return jax.shard_map(body, mesh=torus, in_specs=in_specs, out_specs=out_specs, check_vma=False)
```

```python
import functools
import jax
import jax.numpy as jnp
from jax import lax
from jax.experimental import pallas as pl
from jax.experimental.pallas import tpu as pltpu
from jax.sharding import Mesh
from jax.sharding import PartitionSpec as P

DH = 128
NS_STEPS = 8
REFINE = 2
CHUNK = 256
VMEM = 20 * 2**20
PAIR = 400
SEQ = ("seq_0", "seq_1", "seq_2")
PLANE = ("seq_0", "seq_1")
CORE = "seq_2"

f32 = jnp.float32
bf16 = jnp.bfloat16


def mm(left, right):
    return jnp.dot(left, right, preferred_element_type=f32)


def mm_tn(left, right):
    return lax.dot_general(left, right, (((0,), (0,)), ((), ())), preferred_element_type=f32)


def mm_nt(left, right):
    return lax.dot_general(left, right, (((1,), (1,)), ((), ())), preferred_element_type=f32)


def split(x):
    high = x.astype(bf16)
    return high, (x - high.astype(f32)).astype(bf16)


def side(x):
    return jnp.concatenate(split(x), axis=1)


def doubled(x):
    x = side(x)
    return jnp.concatenate([x, x], axis=0)


def fold(x):
    return x[:, :DH] + x[:, DH:]


def eye():
    rows = lax.broadcasted_iota(jnp.int32, (DH, DH), 0)
    columns = lax.broadcasted_iota(jnp.int32, (DH, DH), 1)
    return (rows == columns).astype(f32)


def scaled_keys(key, gain):
    return (key.astype(f32) * gain).astype(bf16)


def in_hbm(*arrays):
    return [pltpu.with_memory_space_constraint(x, pltpu.HBM) for x in arrays]


def place_of(core_ref, step, heads):
    return lax.rem(step + core_ref[0] * (heads // 2), heads)


def triangles():
    rows = lax.broadcasted_iota(jnp.int32, (DH, DH), 0)
    columns = lax.broadcasted_iota(jnp.int32, (DH, DH), 1)
    return rows <= columns, rows == columns


def gram_kernel(core_ref, gain_ref, reg_ref, k_ref, v_ref, keep_ref, send_ref, local_ref, scaled_ref, ridge_ref):
    step = pl.program_id(0)
    heads = 2 * pl.num_programs(0)
    both = []
    for a in range(2):
        h = place_of(core_ref, 2 * step + a, heads)
        columns = slice(a * DH, (a + 1) * DH)
        k = scaled_keys(k_ref[:, columns], gain_ref[h])
        scaled_ref[:, columns] = k
        ridge_ref[a] = jnp.full(ridge_ref.shape[1:], reg_ref[h])
        pair = jnp.concatenate([k, v_ref[:, columns]], axis=1)
        first = mm_tn(k[:CHUNK], pair[:CHUNK])
        local_ref[a, 0] = first[:, :DH]
        local_ref[a, 1] = first[:, DH:]
        both.append(first + mm_tn(k[CHUNK:], pair[CHUNK:]))
        local_ref[a, 2] = both[a][:, :DH]
    one, two = both[0][:, :DH], both[1][:, :DH]
    above, on = triangles()
    packed = jnp.where(above, one, two)
    diagonal = jnp.sum(jnp.where(on, two, 0.0), axis=0, keepdims=True)

    def put(out_ref):
        for a in range(2):
            out_ref[0, a * DH : (a + 1) * DH] = both[a][:, DH:]
        out_ref[0, 2 * DH : 3 * DH] = packed
        out_ref[0, 3 * DH :] = jnp.broadcast_to(diagonal, (PAIR - 3 * DH, DH))

    @pl.when(step < heads // 4)
    def _():
        put(keep_ref)

    @pl.when(step >= heads // 4)
    def _():
        put(send_ref)


def grams(core, gain, reg, key, value):
    gain, reg, key, value = in_hbm(gain, reg, key, value)
    rows, width = key.shape
    heads = width // DH
    steps = heads // 2
    smem = pl.BlockSpec(memory_space=pltpu.SMEM)
    wide = pl.BlockSpec((rows, 2 * DH), lambda i, c: (0, lax.rem(i + c[0] * (steps // 2), steps)))
    low = pl.BlockSpec((1, PAIR, DH), lambda i, c: (jnp.minimum(i, steps // 2 - 1), 0, 0))
    high = pl.BlockSpec((1, PAIR, DH), lambda i, c: (jnp.maximum(i - steps // 2, 0), 0, 0))
    slabs = jax.ShapeDtypeStruct((steps // 2, PAIR, DH), f32)
    return pl.pallas_call(
        gram_kernel,
        grid_spec=pltpu.PrefetchScalarGridSpec(
            num_scalar_prefetch=1,
            grid=(steps,),
            in_specs=[smem, smem, wide, wide],
            out_specs=[
                low,
                high,
                pl.BlockSpec((2, 3, DH, DH), lambda i, c: (i, 0, 0, 0)),
                wide,
                pl.BlockSpec((2, 8, DH), lambda i, c: (i, 0, 0)),
            ],
        ),
        out_shape=[
            slabs,
            slabs,
            jax.ShapeDtypeStruct((heads, 3, DH, DH), f32),
            jax.ShapeDtypeStruct((rows, width), bf16),
            jax.ShapeDtypeStruct((heads, 8, DH), f32),
        ],
        compiler_params=pltpu.CompilerParams(vmem_limit_bytes=VMEM),
        name="grams",
    )(core, gain, reg, key, value)


def running_kernel(x_ref, o_ref):
    total = x_ref[0]
    o_ref[0] = jnp.zeros_like(total)
    for j in range(1, x_ref.shape[0]):
        o_ref[j] = total
        if j < x_ref.shape[0] - 1:
            total = total + x_ref[j]


def sums_before(pieces):
    return pl.pallas_call(
        running_kernel,
        out_shape=jax.ShapeDtypeStruct(pieces.shape, f32),
        in_specs=[pl.BlockSpec(memory_space=pltpu.VMEM)],
        out_specs=pl.BlockSpec(memory_space=pltpu.VMEM),
        compiler_params=pltpu.CompilerParams(vmem_limit_bytes=VMEM),
        name="sums_before",
    )(pieces)


def newton_schulz(ridge_ref, prior_ref, local_ref, base_ref, y_ref):
    heads = range(local_ref.shape[0])
    inverse, approx, product = {}, {}, {}

    def begin():
        identity = eye()
        above, on = triangles()
        priors = []
        for pair in range(prior_ref.shape[0]):
            packed = prior_ref[pair, 2 * DH : 3 * DH]
            turned = packed.T
            diagonal = prior_ref[pair, 3 * DH : 3 * DH + 1]
            priors.append(jnp.where(above, packed, turned))
            priors.append(jnp.where(on, diagonal, jnp.where(above, turned, packed)))
        for i in heads:
            base = identity * ridge_ref[i, :1] + priors[i]
            base_ref[i] = base
            end = base + local_ref[i, 2]
            squares = jnp.sum(jnp.sum(end * end, axis=0, keepdims=True), axis=1, keepdims=True)
            inverse[i] = 1.0 / jnp.sqrt(squares)
            z = end * inverse[i]
            approx[i] = 2.0 * identity - z
            product[i] = 2.0 * z - fold(mm(side(z), doubled(z)))

    def step():
        for i in heads:
            both = jnp.concatenate([approx[i], product[i]], axis=0)
            both = 2.0 * both - fold(mm(side(both), doubled(product[i])))
            approx[i], product[i] = both[:DH], both[DH:]

    def end():
        for i in heads:
            last = 2.0 * approx[i] - fold(mm(side(approx[i]), doubled(product[i])))
            y_ref[i] = last * inverse[i]

    return [begin] + [step] * (NS_STEPS - 2) + [end]


def diagonal_blocks(two):
    zero = jnp.zeros((DH, DH), two.dtype)
    upper = jnp.concatenate([two[:, :DH], zero], axis=1)
    lower = jnp.concatenate([zero, two[:, DH:]], axis=1)
    return jnp.concatenate([upper, lower], axis=0)


def halves_of(x):
    return x[:, :DH], x[:, DH:]


def beside(parts):
    high, low = (halves_of(x) for x in parts)
    return [jnp.concatenate([high[a], low[a]], axis=1) for a in range(2)]


def solving(half, q_ref, k_ref, v_ref, y_ref, base_ref, prior_ref, local_ref, o_ref):
    rows_in = q_ref.shape[0]
    width = q_ref.shape[1] // 2
    groups, weights = [], {}

    def begin():
        shape = (CHUNK, 2 * DH)
        columns = lax.rem(lax.broadcasted_iota(jnp.int32, shape, 1), DH)
        weights["causal"] = lax.broadcasted_iota(jnp.int32, shape, 0) >= columns
        for p in range(width // (2 * DH)):
            inside = slice(2 * p * DH, 2 * (p + 1) * DH)
            columns = pl.ds(pl.multiple_of(half * width + 2 * p * DH, 2 * DH), 2 * DH)
            group = []
            for a in range(2):
                y = side(y_ref[2 * p + a])
                weights[p, a] = y, jnp.concatenate([y, y], axis=0)
            for j in range(rows_in // CHUNK):
                rows = slice(j * CHUNK, (j + 1) * CHUNK)
                k, v = k_ref[rows, columns], v_ref[rows, columns]
                base, prior = [], []
                for a in range(2):
                    h = 2 * p + a
                    b, c = base_ref[h], prior_ref[p, a * DH : (a + 1) * DH]
                    base.append(doubled(b + local_ref[h, 0] if j else b))
                    prior.append(doubled(c + local_ref[h, 1] if j else c))
                blocks = lambda x: [diagonal_blocks(x[i * DH : (i + 1) * DH]) for i in range(CHUNK // DH)]
                group.append(dict(at=(rows, inside), q=q_ref[rows, columns], k=blocks(k), v=blocks(v), base=base, prior=prior))
            groups.append(group)
        through("s", 0, lambda c: halves_of(c["q"]))

    def through(key, which, rows_of):
        for p, group in enumerate(groups):
            parts = [rows_of(c) for c in group]
            out = []
            for a in range(2):
                rows = jnp.concatenate([x[a] for x in parts], axis=0)
                out.append(fold(mm(rows, weights[p, a][which])))
            for n, c in enumerate(group):
                c[key] = jnp.concatenate([x[n * CHUNK : (n + 1) * CHUNK] for x in out], axis=1)

    def each(function):
        def run():
            for group in groups:
                for c in group:
                    function(c)

        return run

    def score(c):
        c["parts"] = split(c["s"])
        high = c["parts"][0]
        c["scores"] = []
        for i, k in enumerate(c["k"]):
            scores = mm_nt(high[i * DH :], k)
            causal = weights["causal"][: CHUNK - i * DH]
            c["scores"].append(jnp.where(causal, scores, 0.0).astype(bf16))

    def times(c, matrices):
        rows = beside(c["parts"])
        return jnp.concatenate([fold(mm(rows[a], matrices[a])) for a in range(2)], axis=1)

    def inside(c, values):
        first = mm(c["scores"][0], values[0])
        return jnp.concatenate([first[:DH], first[DH:] + mm(c["scores"][1], values[1])], axis=0)

    def residual(c):
        c["residual"] = c["q"].astype(f32) - times(c, c["base"]) - inside(c, c["k"])

    def correct():
        through("step", 1, lambda c: beside(split(c["residual"])))
        for group in groups:
            for c in group:
                c["s"] = c["s"] + c["step"]

    def readout(c):
        o_ref[c["at"]] = (times(c, c["prior"]) + inside(c, c["v"])).astype(bf16)

    return [begin] + [each(score), each(residual), correct] * REFINE + [each(score), each(readout)]


def precond_kernel(ridge_ref, prior_ref, local_ref, base_ref, y_ref):
    for step in newton_schulz(ridge_ref, prior_ref, local_ref, base_ref, y_ref):
        step()


def first_kernel(
    core_ref, q_ref, k_ref, v_ref, y_ref, base_ref, prior_ref, local_ref,
    ridge_ref, later_prior_ref, later_local_ref, o_ref, later_base_ref, later_y_ref,
):
    mine = solving(core_ref[0], q_ref, k_ref, v_ref, y_ref, base_ref, prior_ref, local_ref, o_ref)
    later = newton_schulz(ridge_ref, later_prior_ref, later_local_ref, later_base_ref, later_y_ref)
    for i in range(max(len(mine), len(later))):
        for steps in (mine, later):
            if i < len(steps):
                steps[i]()


def second_kernel(core_ref, q_ref, k_ref, v_ref, y_ref, base_ref, prior_ref, local_ref, done_ref, o_ref):
    for step in solving(1 - core_ref[0], q_ref, k_ref, v_ref, y_ref, base_ref, prior_ref, local_ref, o_ref):
        step()


WHOLE = pl.BlockSpec(memory_space=pltpu.VMEM)


def part_of(shape, at):
    return pl.BlockSpec(shape, lambda i, c: (at,) + (0,) * (len(shape) - 1))


def call(kernel, core, args, in_specs, out_specs, out_shape, name, **options):
    return pl.pallas_call(
        kernel,
        grid_spec=pltpu.PrefetchScalarGridSpec(
            num_scalar_prefetch=1, grid=(1,), in_specs=in_specs, out_specs=out_specs
        ),
        out_shape=out_shape,
        compiler_params=pltpu.CompilerParams(vmem_limit_bytes=VMEM),
        name=name,
        **options,
    )(core, *args)


def halves(heads):
    shape = jax.ShapeDtypeStruct((heads // 2, DH, DH), f32)
    return [shape, shape]


def precond_first_kernel(core_ref, *refs):
    precond_kernel(*refs)


def preconditioners(core, ridge, prior, local):
    heads = local.shape[0]
    block = (heads // 2,)
    return call(
        precond_first_kernel,
        core,
        (ridge, prior, local),
        [part_of(block + ridge.shape[1:], 0), WHOLE, part_of(block + local.shape[1:], 0)],
        [WHOLE, WHOLE],
        halves(heads),
        "preconditioners",
        cost_estimate=pl.CostEstimate(flops=10**9, bytes_accessed=2 * 10**6, transcendentals=0),
    )


def first_solve(core, query, key, value, y, base, prior, local, ridge, later):
    rows, width = query.shape
    heads = local.shape[0]
    block = (heads // 2,)
    return call(
        first_kernel,
        core,
        (query, key, value, y, base, prior, local, ridge, later, local),
        [WHOLE] * 6
        + [part_of(block + local.shape[1:], 0), part_of(block + ridge.shape[1:], 1), WHOLE]
        + [part_of(block + local.shape[1:], 1)],
        [pl.BlockSpec((rows, width // 2), lambda i, c: (0, c[0])), WHOLE, WHOLE],
        [jax.ShapeDtypeStruct((rows, width), bf16)] + halves(heads),
        "first_solve",
        cost_estimate=pl.CostEstimate(flops=3 * 10**9, bytes_accessed=2 * 10**6, transcendentals=0),
    )


def second_solve(core, query, key, value, y, base, prior, local, done):
    rows, width = query.shape
    block = (local.shape[0] // 2,)
    return call(
        second_kernel,
        core,
        (query, key, value, y, base, prior, local, done),
        [WHOLE] * 6 + [part_of(block + local.shape[1:], 1), pl.BlockSpec(memory_space=pl.ANY)],
        pl.BlockSpec((rows, width // 2), lambda i, c: (0, 1 - c[0])),
        jax.ShapeDtypeStruct((rows, width), bf16),
        "second_solve",
        input_output_aliases={8: 0},
    )


def exchange(x):
    return lax.all_to_all(x, PLANE, 0, 0)


def swapped(x):
    return lax.ppermute(x, CORE, [(0, 1), (1, 0)])


def body(query_rows, key_rows, value_rows, key_gain, regularizer):
    place = lax.axis_index(CORE)
    core = place.astype(jnp.int32).reshape(1)
    chips = lax.axis_size(PLANE)
    core, is_first, is_second = lax.optimization_barrier((core, place == 0, place == 1))
    keep, send, local, scaled, ridge = grams(core, key_gain, regularizer, key_rows, value_rows)
    received = swapped(send)
    pieces = exchange((keep + received).reshape(chips, 1, -1))
    before = exchange(sums_before(pieces)).reshape(keep.shape)
    mine = before + jnp.where(is_second, received, 0.0)
    other = swapped(before + jnp.where(is_first, keep, 0.0))
    base, y = preconditioners(core, ridge, mine, local)
    done, base1, y1 = first_solve(
        core, query_rows, scaled, value_rows, y, base, mine, local, ridge, other
    )
    return second_solve(core, query_rows, scaled, value_rows, y1, base1, other, local, done)


def solution(mesh):
    torus = Mesh(
        mesh.devices.reshape(8, 4, 2, mesh.shape["head"]), ("seq_0", "seq_1", "seq_2", "head")
    )
    in_specs = (P(SEQ, "head"), P(SEQ, "head"), P(SEQ, "head"), P("head"), P("head"))
    out_specs = P(SEQ, "head")
    return jax.shard_map(body, mesh=torus, in_specs=in_specs, out_specs=out_specs, check_vma=False)
```

```python
import functools
import jax
import jax.numpy as jnp
from jax import lax
from jax.experimental import pallas as pl
from jax.experimental.pallas import tpu as pltpu
from jax.sharding import Mesh
from jax.sharding import PartitionSpec as P

DH = 128
NS_STEPS = 8
REFINE = 2
CHUNK = 256
VMEM = 20 * 2**20
PAIR = 400
SEQ = ("seq_0", "seq_1", "seq_2")
PLANE = ("seq_0", "seq_1")
CORE = "seq_2"

f32 = jnp.float32
bf16 = jnp.bfloat16


def mm(left, right):
    return jnp.dot(left, right, preferred_element_type=f32)


def mm_tn(left, right):
    return lax.dot_general(left, right, (((0,), (0,)), ((), ())), preferred_element_type=f32)


def mm_nt(left, right):
    return lax.dot_general(left, right, (((1,), (1,)), ((), ())), preferred_element_type=f32)


def split(x):
    high = x.astype(bf16)
    return high, (x - high.astype(f32)).astype(bf16)


def side(x):
    return jnp.concatenate(split(x), axis=1)


def doubled(x):
    x = side(x)
    return jnp.concatenate([x, x], axis=0)


def fold(x):
    return x[:, :DH] + x[:, DH:]


def eye():
    rows = lax.broadcasted_iota(jnp.int32, (DH, DH), 0)
    columns = lax.broadcasted_iota(jnp.int32, (DH, DH), 1)
    return (rows == columns).astype(f32)


def scaled_keys(key, gain):
    return (key.astype(f32) * gain).astype(bf16)


def in_hbm(*arrays):
    return [pltpu.with_memory_space_constraint(x, pltpu.HBM) for x in arrays]


def triangles():
    rows = lax.broadcasted_iota(jnp.int32, (DH, DH), 0)
    columns = lax.broadcasted_iota(jnp.int32, (DH, DH), 1)
    return rows <= columns, rows == columns


def gram_kernel(which, core_ref, gain_ref, reg_ref, k_ref, v_ref, slab_ref, local_ref, scaled_ref, ridge_ref):
    half = 1 - core_ref[0] if which else core_ref[0]
    both = []
    for a in range(2):
        h = 2 * (half * pl.num_programs(0) + pl.program_id(0)) + a
        columns = slice(a * DH, (a + 1) * DH)
        k = scaled_keys(k_ref[:, columns], gain_ref[h])
        scaled_ref[:, columns] = k
        ridge_ref[a] = jnp.full(ridge_ref.shape[1:], reg_ref[h])
        pair = jnp.concatenate([k, v_ref[:, columns]], axis=1)
        first = mm_tn(k[:CHUNK], pair[:CHUNK])
        local_ref[a, 0] = first[:, :DH]
        local_ref[a, 1] = first[:, DH:]
        both.append(first + mm_tn(k[CHUNK:], pair[CHUNK:]))
        local_ref[a, 2] = both[a][:, :DH]
    one, two = both[0][:, :DH], both[1][:, :DH]
    above, on = triangles()
    for a in range(2):
        slab_ref[0, a * DH : (a + 1) * DH] = both[a][:, DH:]
    slab_ref[0, 2 * DH : 3 * DH] = jnp.where(above, one, two)
    diagonal = jnp.sum(jnp.where(on, two, 0.0), axis=0, keepdims=True)
    slab_ref[0, 3 * DH :] = jnp.broadcast_to(diagonal, (PAIR - 3 * DH, DH))


def grams(which, core, gain, reg, key, value):
    gain, reg, key, value = in_hbm(gain, reg, key, value)
    rows, width = key.shape
    steps = width // DH // 4
    smem = pl.BlockSpec(memory_space=pltpu.SMEM)
    wide = pl.BlockSpec((rows, 2 * DH), lambda i, c: (0, i + steps * (1 - c[0] if which else c[0])))
    return pl.pallas_call(
        functools.partial(gram_kernel, which),
        grid_spec=pltpu.PrefetchScalarGridSpec(
            num_scalar_prefetch=1,
            grid=(steps,),
            in_specs=[smem, smem, wide, wide],
            out_specs=[
                pl.BlockSpec((1, PAIR, DH), lambda i, c: (i, 0, 0)),
                pl.BlockSpec((2, 3, DH, DH), lambda i, c: (i, 0, 0, 0)),
                pl.BlockSpec((rows, 2 * DH), lambda i, c: (0, i)),
                pl.BlockSpec((2, 8, DH), lambda i, c: (i, 0, 0)),
            ],
        ),
        out_shape=[
            jax.ShapeDtypeStruct((steps, PAIR, DH), f32),
            jax.ShapeDtypeStruct((2 * steps, 3, DH, DH), f32),
            jax.ShapeDtypeStruct((rows, width // 2), bf16),
            jax.ShapeDtypeStruct((2 * steps, 8, DH), f32),
        ],
        compiler_params=pltpu.CompilerParams(vmem_limit_bytes=VMEM),
        cost_estimate=pl.CostEstimate(flops=10**9, bytes_accessed=2 * 10**6, transcendentals=0),
        name=f"grams_{which}",
    )(core, gain, reg, key, value)


def running_kernel(x_ref, o_ref):
    total = x_ref[0]
    o_ref[0] = jnp.zeros_like(total)
    for j in range(1, x_ref.shape[0]):
        o_ref[j] = total
        if j < x_ref.shape[0] - 1:
            total = total + x_ref[j]


def sums_before(pieces):
    return pl.pallas_call(
        running_kernel,
        out_shape=jax.ShapeDtypeStruct(pieces.shape, f32),
        in_specs=[pl.BlockSpec(memory_space=pltpu.VMEM)],
        out_specs=pl.BlockSpec(memory_space=pltpu.VMEM),
        compiler_params=pltpu.CompilerParams(vmem_limit_bytes=VMEM),
        name="sums_before",
    )(pieces)


def newton_schulz(ridge_ref, prior_ref, local_ref, base_ref, y_ref):
    heads = range(local_ref.shape[0])
    inverse, approx, product = {}, {}, {}

    def begin():
        identity = eye()
        above, on = triangles()
        priors = []
        for pair in range(prior_ref.shape[0]):
            packed = prior_ref[pair, 2 * DH : 3 * DH]
            turned = packed.T
            diagonal = prior_ref[pair, 3 * DH : 3 * DH + 1]
            priors.append(jnp.where(above, packed, turned))
            priors.append(jnp.where(on, diagonal, jnp.where(above, turned, packed)))
        for i in heads:
            base = identity * ridge_ref[i, :1] + priors[i]
            base_ref[i] = base
            end = base + local_ref[i, 2]
            squares = jnp.sum(jnp.sum(end * end, axis=0, keepdims=True), axis=1, keepdims=True)
            inverse[i] = 1.0 / jnp.sqrt(squares)
            z = end * inverse[i]
            approx[i] = 2.0 * identity - z
            product[i] = 2.0 * z - fold(mm(side(z), doubled(z)))

    def step():
        for i in heads:
            both = jnp.concatenate([approx[i], product[i]], axis=0)
            both = 2.0 * both - fold(mm(side(both), doubled(product[i])))
            approx[i], product[i] = both[:DH], both[DH:]

    def end():
        for i in heads:
            last = 2.0 * approx[i] - fold(mm(side(approx[i]), doubled(product[i])))
            y_ref[i] = last * inverse[i]

    return [begin] + [step] * (NS_STEPS - 2) + [end]


def diagonal_blocks(two):
    zero = jnp.zeros((DH, DH), two.dtype)
    upper = jnp.concatenate([two[:, :DH], zero], axis=1)
    lower = jnp.concatenate([zero, two[:, DH:]], axis=1)
    return jnp.concatenate([upper, lower], axis=0)


def halves_of(x):
    return x[:, :DH], x[:, DH:]


def beside(parts):
    high, low = (halves_of(x) for x in parts)
    return [jnp.concatenate([high[a], low[a]], axis=1) for a in range(2)]


def solving(half, q_ref, k_ref, v_ref, y_ref, base_ref, prior_ref, local_ref, o_ref, written=None):
    rows_in = q_ref.shape[0]
    width = q_ref.shape[1] // 2
    groups, weights = [], {}

    def begin():
        shape = (CHUNK, 2 * DH)
        columns = lax.rem(lax.broadcasted_iota(jnp.int32, shape, 1), DH)
        weights["causal"] = lax.broadcasted_iota(jnp.int32, shape, 0) >= columns
        for p in range(width // (2 * DH)):
            inside = slice(2 * p * DH, 2 * (p + 1) * DH)
            columns = pl.ds(pl.multiple_of(half * width + 2 * p * DH, 2 * DH), 2 * DH)
            group = []
            for a in range(2):
                y = side(y_ref[2 * p + a])
                weights[p, a] = y, jnp.concatenate([y, y], axis=0)
            for j in range(rows_in // CHUNK):
                rows = slice(j * CHUNK, (j + 1) * CHUNK)
                k, v = k_ref[rows, inside], v_ref[rows, columns]
                base, prior = [], []
                for a in range(2):
                    h = 2 * p + a
                    b, c = base_ref[h], prior_ref[p, a * DH : (a + 1) * DH]
                    base.append(doubled(b + local_ref[h, 0] if j else b))
                    prior.append(doubled(c + local_ref[h, 1] if j else c))
                blocks = lambda x: [diagonal_blocks(x[i * DH : (i + 1) * DH]) for i in range(CHUNK // DH)]
                group.append(dict(at=(rows, inside), q=q_ref[rows, columns], k=blocks(k), v=blocks(v), base=base, prior=prior))
            groups.append(group)
        through("s", 0, lambda c: halves_of(c["q"]))

    def through(key, which, rows_of):
        for p, group in enumerate(groups):
            parts = [rows_of(c) for c in group]
            out = []
            for a in range(2):
                rows = jnp.concatenate([x[a] for x in parts], axis=0)
                out.append(fold(mm(rows, weights[p, a][which])))
            for n, c in enumerate(group):
                c[key] = jnp.concatenate([x[n * CHUNK : (n + 1) * CHUNK] for x in out], axis=1)

    def each(function):
        def run():
            for group in groups:
                for c in group:
                    function(c)

        return run

    def score(c):
        c["parts"] = split(c["s"])
        high = c["parts"][0]
        c["scores"] = []
        for i, k in enumerate(c["k"]):
            scores = mm_nt(high[i * DH :], k)
            causal = weights["causal"][: CHUNK - i * DH]
            c["scores"].append(jnp.where(causal, scores, 0.0).astype(bf16))

    def times(c, matrices):
        rows = beside(c["parts"])
        return jnp.concatenate([fold(mm(rows[a], matrices[a])) for a in range(2)], axis=1)

    def causal_sum(c, values):
        first = mm(c["scores"][0], values[0])
        return jnp.concatenate([first[:DH], first[DH:] + mm(c["scores"][1], values[1])], axis=0)

    def residual(c):
        c["residual"] = c["q"].astype(f32) - times(c, c["base"]) - causal_sum(c, c["k"])

    def correct():
        through("step", 1, lambda c: beside(split(c["residual"])))
        for group in groups:
            for c in group:
                c["s"] = c["s"] + c["step"]

    def readout(c):
        o_ref[c["at"]] = (times(c, c["prior"]) + causal_sum(c, c["v"])).astype(bf16)
        if written is not None:
            written(c["at"])

    return [begin] + [each(score), each(residual), correct] * REFINE + [each(score), each(readout)]


def precond_kernel(ridge_ref, prior_ref, local_ref, base_ref, y_ref):
    for step in newton_schulz(ridge_ref, prior_ref, local_ref, base_ref, y_ref):
        step()


def first_kernel(
    core_ref, q_ref, k_ref, v_ref, y_ref, base_ref, prior_ref, local_ref,
    ridge_ref, later_prior_ref, later_local_ref, o_ref, later_base_ref, later_y_ref,
):
    mine = solving(core_ref[0], q_ref, k_ref, v_ref, y_ref, base_ref, prior_ref, local_ref, o_ref)
    later = newton_schulz(ridge_ref, later_prior_ref, later_local_ref, later_base_ref, later_y_ref)
    for i in range(max(len(mine), len(later))):
        for steps in (mine, later):
            if i < len(steps):
                steps[i]()


def second_kernel(
    core_ref, q_ref, k_ref, v_ref, y_ref, base_ref, prior_ref, local_ref, done_ref, o_ref, out_ref, sems
):
    width = done_ref.shape[1]
    half = 1 - core_ref[0]
    copies = []

    def send(source, rows, start, size, number):
        columns = pl.ds(pl.multiple_of(start, 2 * DH), size)
        copies.append(pltpu.make_async_copy(source, o_ref.at[rows, columns], sems.at[number]))
        copies[-1].start()

    def written(at):
        rows, columns = at
        size = columns.stop - columns.start
        send(out_ref.at[rows, columns], rows, half * width + columns.start, size, len(copies))

    send(done_ref, slice(None), core_ref[0] * width, width, 0)
    for step in solving(half, q_ref, k_ref, v_ref, y_ref, base_ref, prior_ref, local_ref, out_ref, written):
        step()
    for copy in copies:
        copy.wait()


WHOLE = pl.BlockSpec(memory_space=pltpu.VMEM)


def call(kernel, core, args, out_specs, out_shape, name, flops, scratch=()):
    return pl.pallas_call(
        kernel,
        grid_spec=pltpu.PrefetchScalarGridSpec(
            num_scalar_prefetch=1, grid=(1,), in_specs=[WHOLE] * len(args), out_specs=out_specs,
            scratch_shapes=scratch,
        ),
        out_shape=out_shape,
        compiler_params=pltpu.CompilerParams(vmem_limit_bytes=VMEM),
        cost_estimate=pl.CostEstimate(flops=flops, bytes_accessed=2 * 10**6, transcendentals=0),
        name=name,
    )(core, *args)


def precond_first_kernel(core_ref, *refs):
    precond_kernel(*refs)


def matrices_like(local):
    return jax.ShapeDtypeStruct((local.shape[0], DH, DH), f32)


def preconditioners(core, ridge, prior, local):
    shape = matrices_like(local)
    args = (ridge, prior, local)
    return call(precond_first_kernel, core, args, [WHOLE] * 2, [shape] * 2, "preconditioners", 10**9)


def first_solve(core, query, key, value, y, base, prior, local, ridge, later, later_local):
    shape = matrices_like(local)
    args = (query, key, value, y, base, prior, local, ridge, later, later_local)
    out = jax.ShapeDtypeStruct(key.shape, bf16)
    return call(first_kernel, core, args, [WHOLE] * 3, [out, shape, shape], "first_solve", 3 * 10**9)


def second_solve(core, query, key, value, y, base, prior, local, done):
    args = (query, key, value, y, base, prior, local, done)
    out = jax.ShapeDtypeStruct(query.shape, bf16)
    units = query.shape[0] // CHUNK * (key.shape[1] // (2 * DH))
    scratch = [pltpu.VMEM(key.shape, bf16), pltpu.SemaphoreType.DMA((units + 1,))]
    spec = pl.BlockSpec(memory_space=pltpu.HBM)
    return call(second_kernel, core, args, spec, out, "second_solve", 3 * 10**9, scratch)


def exchange(x):
    return lax.all_to_all(x, PLANE, 0, 0)


def swapped(x):
    return lax.ppermute(x, CORE, [(0, 1), (1, 0)])


def body(query_rows, key_rows, value_rows, key_gain, regularizer):
    place = lax.axis_index(CORE)
    core = place.astype(jnp.int32).reshape(1)
    chips = lax.axis_size(PLANE)
    core, is_first, is_second = lax.optimization_barrier((core, place == 0, place == 1))
    send, local1, scaled1, ridge1 = grams(1, core, key_gain, regularizer, key_rows, value_rows)
    received = swapped(send)
    keep, local0, scaled0, ridge0 = grams(0, core, key_gain, regularizer, key_rows, value_rows)
    pieces = exchange((keep + received).reshape(chips, 1, -1))
    before = exchange(sums_before(pieces)).reshape(keep.shape)
    mine = before + jnp.where(is_second, received, 0.0)
    other = swapped(before + jnp.where(is_first, keep, 0.0))
    base, y = preconditioners(core, ridge0, mine, local0)
    done, base1, y1 = first_solve(
        core, query_rows, scaled0, value_rows, y, base, mine, local0, ridge1, other, local1
    )
    return second_solve(core, query_rows, scaled1, value_rows, y1, base1, other, local1, done)


def solution(mesh):
    torus = Mesh(
        mesh.devices.reshape(8, 4, 2, mesh.shape["head"]), ("seq_0", "seq_1", "seq_2", "head")
    )
    in_specs = (P(SEQ, "head"), P(SEQ, "head"), P(SEQ, "head"), P("head"), P("head"))
    out_specs = P(SEQ, "head")
    return jax.shard_map(body, mesh=torus, in_specs=in_specs, out_specs=out_specs, check_vma=False)
```

```python
import functools
import jax
import jax.numpy as jnp
from jax import lax
from jax.experimental import pallas as pl
from jax.experimental.pallas import tpu as pltpu
from jax.sharding import Mesh
from jax.sharding import PartitionSpec as P

DH = 128
NS_STEPS = 8
REFINE = 2
CHUNK = 256
VMEM = 20 * 2**20
PAIR = 400
SEQ = ("seq_0", "seq_1", "seq_2")
PLANE = ("seq_1", "seq_0")
CORE = "seq_2"

f32 = jnp.float32
bf16 = jnp.bfloat16


def mm(left, right):
    return jnp.dot(left, right, preferred_element_type=f32)


def mm_tn(left, right):
    return lax.dot_general(left, right, (((0,), (0,)), ((), ())), preferred_element_type=f32)


def mm_nt(left, right):
    return lax.dot_general(left, right, (((1,), (1,)), ((), ())), preferred_element_type=f32)


def split(x):
    high = x.astype(bf16)
    return high, (x - high.astype(f32)).astype(bf16)


def side(x):
    return jnp.concatenate(split(x), axis=1)


def doubled(x):
    x = side(x)
    return jnp.concatenate([x, x], axis=0)


def fold(x):
    return x[:, :DH] + x[:, DH:]


def eye():
    rows = lax.broadcasted_iota(jnp.int32, (DH, DH), 0)
    columns = lax.broadcasted_iota(jnp.int32, (DH, DH), 1)
    return (rows == columns).astype(f32)


def scaled_keys(key, gain):
    return (key.astype(f32) * gain).astype(bf16)


def in_hbm(*arrays):
    return [pltpu.with_memory_space_constraint(x, pltpu.HBM) for x in arrays]


def triangles():
    rows = lax.broadcasted_iota(jnp.int32, (DH, DH), 0)
    columns = lax.broadcasted_iota(jnp.int32, (DH, DH), 1)
    return rows <= columns, rows == columns


def gram_kernel(which, core_ref, gain_ref, reg_ref, k_ref, v_ref, slab_ref, local_ref, scaled_ref, ridge_ref):
    half = 1 - core_ref[0] if which else core_ref[0]
    both = []
    for a in range(2):
        h = 2 * (half * pl.num_programs(0) + pl.program_id(0)) + a
        columns = slice(a * DH, (a + 1) * DH)
        k = scaled_keys(k_ref[:, columns], gain_ref[h])
        scaled_ref[:, columns] = k
        ridge_ref[a] = jnp.full(ridge_ref.shape[1:], reg_ref[h])
        pair = jnp.concatenate([k, v_ref[:, columns]], axis=1)
        first = mm_tn(k[:CHUNK], pair[:CHUNK])
        local_ref[a, 0] = first[:, :DH]
        local_ref[a, 1] = first[:, DH:]
        both.append(first + mm_tn(k[CHUNK:], pair[CHUNK:]))
        local_ref[a, 2] = both[a][:, :DH]
    one, two = both[0][:, :DH], both[1][:, :DH]
    above, on = triangles()
    for a in range(2):
        slab_ref[0, a * DH : (a + 1) * DH] = both[a][:, DH:]
    slab_ref[0, 2 * DH : 3 * DH] = jnp.where(above, one, two)
    diagonal = jnp.sum(jnp.where(on, two, 0.0), axis=0, keepdims=True)
    slab_ref[0, 3 * DH :] = jnp.broadcast_to(diagonal, (PAIR - 3 * DH, DH))


def grams(which, core, gain, reg, key, value):
    gain, reg, key, value = in_hbm(gain, reg, key, value)
    rows, width = key.shape
    steps = width // DH // 4
    smem = pl.BlockSpec(memory_space=pltpu.SMEM)
    wide = pl.BlockSpec((rows, 2 * DH), lambda i, c: (0, i + steps * (1 - c[0] if which else c[0])))
    return pl.pallas_call(
        functools.partial(gram_kernel, which),
        grid_spec=pltpu.PrefetchScalarGridSpec(
            num_scalar_prefetch=1,
            grid=(steps,),
            in_specs=[smem, smem, wide, wide],
            out_specs=[
                pl.BlockSpec((1, PAIR, DH), lambda i, c: (i, 0, 0)),
                pl.BlockSpec((2, 3, DH, DH), lambda i, c: (i, 0, 0, 0)),
                pl.BlockSpec((rows, 2 * DH), lambda i, c: (0, i)),
                pl.BlockSpec((2, 8, DH), lambda i, c: (i, 0, 0)),
            ],
        ),
        out_shape=[
            jax.ShapeDtypeStruct((steps, PAIR, DH), f32),
            jax.ShapeDtypeStruct((2 * steps, 3, DH, DH), f32),
            jax.ShapeDtypeStruct((rows, width // 2), bf16),
            jax.ShapeDtypeStruct((2 * steps, 8, DH), f32),
        ],
        compiler_params=pltpu.CompilerParams(vmem_limit_bytes=VMEM),
        cost_estimate=pl.CostEstimate(flops=10**9, bytes_accessed=2 * 10**6, transcendentals=0),
        name=f"grams_{which}",
    )(core, gain, reg, key, value)


def running_kernel(row, x_ref, o_ref):
    line = x_ref.shape[0] // row
    order = [y * line + z for z in range(line) for y in range(row)]
    total = x_ref[0]
    o_ref[0] = jnp.zeros_like(total)
    for j in order[1:]:
        o_ref[j] = total
        if j != order[-1]:
            total = total + x_ref[j]


def sums_before(pieces):
    return pl.pallas_call(
        functools.partial(running_kernel, lax.axis_size(PLANE[0])),
        out_shape=jax.ShapeDtypeStruct(pieces.shape, f32),
        in_specs=[pl.BlockSpec(memory_space=pltpu.VMEM)],
        out_specs=pl.BlockSpec(memory_space=pltpu.VMEM),
        compiler_params=pltpu.CompilerParams(vmem_limit_bytes=VMEM),
        name="sums_before",
    )(pieces)


def newton_schulz(ridge_ref, prior_ref, local_ref, base_ref, y_ref):
    heads = range(local_ref.shape[0])
    inverse, approx, product = {}, {}, {}

    def begin():
        identity = eye()
        above, on = triangles()
        priors = []
        for pair in range(prior_ref.shape[0]):
            packed = prior_ref[pair, 2 * DH : 3 * DH]
            turned = packed.T
            diagonal = prior_ref[pair, 3 * DH : 3 * DH + 1]
            priors.append(jnp.where(above, packed, turned))
            priors.append(jnp.where(on, diagonal, jnp.where(above, turned, packed)))
        for i in heads:
            base = identity * ridge_ref[i, :1] + priors[i]
            base_ref[i] = base
            end = base + local_ref[i, 2]
            squares = jnp.sum(jnp.sum(end * end, axis=0, keepdims=True), axis=1, keepdims=True)
            inverse[i] = 1.0 / jnp.sqrt(squares)
            z = end * inverse[i]
            approx[i] = 2.0 * identity - z
            product[i] = 2.0 * z - fold(mm(side(z), doubled(z)))

    def step():
        for i in heads:
            rows = side(product[i])
            weights = jnp.concatenate([rows, rows], axis=0)
            both = fold(mm(jnp.concatenate([rows, side(approx[i])], axis=0), weights))
            product[i], approx[i] = 2.0 * product[i] - both[:DH], 2.0 * approx[i] - both[DH:]

    def end():
        for i in heads:
            last = 2.0 * approx[i] - fold(mm(side(approx[i]), doubled(product[i])))
            y_ref[i] = last * inverse[i]

    return [begin] + [step] * (NS_STEPS - 2) + [end]


def diagonal_blocks(two):
    zero = jnp.zeros((DH, DH), two.dtype)
    upper = jnp.concatenate([two[:, :DH], zero], axis=1)
    lower = jnp.concatenate([zero, two[:, DH:]], axis=1)
    return jnp.concatenate([upper, lower], axis=0)


def halves_of(x):
    return x[:, :DH], x[:, DH:]


def beside(parts):
    high, low = (halves_of(x) for x in parts)
    return [jnp.concatenate([high[a], low[a]], axis=1) for a in range(2)]


def solving(half, q_ref, k_ref, v_ref, y_ref, base_ref, prior_ref, local_ref, o_ref, written=None):
    rows_in = q_ref.shape[0]
    width = q_ref.shape[1] // 2
    groups, weights = [], {}

    def begin():
        shape = (CHUNK, 2 * DH)
        columns = lax.rem(lax.broadcasted_iota(jnp.int32, shape, 1), DH)
        weights["causal"] = lax.broadcasted_iota(jnp.int32, shape, 0) >= columns
        for p in range(width // (2 * DH)):
            inside = slice(2 * p * DH, 2 * (p + 1) * DH)
            columns = pl.ds(pl.multiple_of(half * width + 2 * p * DH, 2 * DH), 2 * DH)
            group = []
            for a in range(2):
                y = side(y_ref[2 * p + a])
                weights[p, a] = y, jnp.concatenate([y, y], axis=0)
            for j in range(rows_in // CHUNK):
                rows = slice(j * CHUNK, (j + 1) * CHUNK)
                k, v = k_ref[rows, inside], v_ref[rows, columns]
                base, prior = [], []
                for a in range(2):
                    h = 2 * p + a
                    b, c = base_ref[h], prior_ref[p, a * DH : (a + 1) * DH]
                    base.append(doubled(b + local_ref[h, 0] if j else b))
                    prior.append(doubled(c + local_ref[h, 1] if j else c))
                blocks = lambda x: [diagonal_blocks(x[i * DH : (i + 1) * DH]) for i in range(CHUNK // DH)]
                group.append(dict(at=(rows, inside), q=q_ref[rows, columns], k=blocks(k), v=blocks(v), base=base, prior=prior))
            groups.append(group)
        through("s", 0, lambda c: halves_of(c["q"]))

    def through(key, which, rows_of):
        for p, group in enumerate(groups):
            parts = [rows_of(c) for c in group]
            out = []
            for a in range(2):
                rows = jnp.concatenate([x[a] for x in parts], axis=0)
                out.append(fold(mm(rows, weights[p, a][which])))
            for n, c in enumerate(group):
                c[key] = jnp.concatenate([x[n * CHUNK : (n + 1) * CHUNK] for x in out], axis=1)

    def each(function):
        def run():
            for group in groups:
                for c in group:
                    function(c)

        return run

    def score(c):
        c["parts"] = split(c["s"])
        high = c["parts"][0]
        c["scores"] = []
        for i, k in enumerate(c["k"]):
            scores = mm_nt(high[i * DH :], k)
            causal = weights["causal"][: CHUNK - i * DH]
            c["scores"].append(jnp.where(causal, scores, 0.0).astype(bf16))

    def times(c, matrices):
        rows = beside(c["parts"])
        return jnp.concatenate([fold(mm(rows[a], matrices[a])) for a in range(2)], axis=1)

    def causal_sum(c, values):
        first = mm(c["scores"][0], values[0])
        return jnp.concatenate([first[:DH], first[DH:] + mm(c["scores"][1], values[1])], axis=0)

    def residual(c):
        c["residual"] = c["q"].astype(f32) - times(c, c["base"]) - causal_sum(c, c["k"])

    def correct():
        through("step", 1, lambda c: beside(split(c["residual"])))
        for group in groups:
            for c in group:
                c["s"] = c["s"] + c["step"]

    def readout(c):
        o_ref[c["at"]] = (times(c, c["prior"]) + causal_sum(c, c["v"])).astype(bf16)
        if written is not None:
            written(c["at"])

    return [begin] + [each(score), each(residual), correct] * REFINE + [each(score), each(readout)]


def precond_kernel(ridge_ref, prior_ref, local_ref, base_ref, y_ref):
    for step in newton_schulz(ridge_ref, prior_ref, local_ref, base_ref, y_ref):
        step()


def first_kernel(
    core_ref, q_ref, k_ref, v_ref, y_ref, base_ref, prior_ref, local_ref,
    ridge_ref, later_prior_ref, later_local_ref, o_ref, later_base_ref, later_y_ref,
):
    mine = solving(core_ref[0], q_ref, k_ref, v_ref, y_ref, base_ref, prior_ref, local_ref, o_ref)
    later = newton_schulz(ridge_ref, later_prior_ref, later_local_ref, later_base_ref, later_y_ref)
    for i in range(max(len(mine), len(later))):
        for steps in (mine, later):
            if i < len(steps):
                steps[i]()


def second_kernel(
    core_ref, q_ref, k_ref, v_ref, y_ref, base_ref, prior_ref, local_ref, done_ref, o_ref, out_ref, sems
):
    width = done_ref.shape[1]
    half = 1 - core_ref[0]
    copies = []

    def send(source, rows, start, size, number):
        columns = pl.ds(pl.multiple_of(start, 2 * DH), size)
        copies.append(pltpu.make_async_copy(source, o_ref.at[rows, columns], sems.at[number]))
        copies[-1].start()

    def written(at):
        rows, columns = at
        size = columns.stop - columns.start
        send(out_ref.at[rows, columns], rows, half * width + columns.start, size, len(copies))

    send(done_ref, slice(None), core_ref[0] * width, width, 0)
    for step in solving(half, q_ref, k_ref, v_ref, y_ref, base_ref, prior_ref, local_ref, out_ref, written):
        step()
    for copy in copies:
        copy.wait()


WHOLE = pl.BlockSpec(memory_space=pltpu.VMEM)


def call(kernel, core, args, out_specs, out_shape, name, flops, scratch=()):
    return pl.pallas_call(
        kernel,
        grid_spec=pltpu.PrefetchScalarGridSpec(
            num_scalar_prefetch=1, grid=(1,), in_specs=[WHOLE] * len(args), out_specs=out_specs,
            scratch_shapes=scratch,
        ),
        out_shape=out_shape,
        compiler_params=pltpu.CompilerParams(vmem_limit_bytes=VMEM),
        cost_estimate=pl.CostEstimate(flops=flops, bytes_accessed=2 * 10**6, transcendentals=0),
        name=name,
    )(core, *args)


def precond_first_kernel(core_ref, *refs):
    precond_kernel(*refs)


def matrices_like(local):
    return jax.ShapeDtypeStruct((local.shape[0], DH, DH), f32)


def preconditioners(core, ridge, prior, local):
    shape = matrices_like(local)
    args = (ridge, prior, local)
    return call(precond_first_kernel, core, args, [WHOLE] * 2, [shape] * 2, "preconditioners", 10**9)


def first_solve(core, query, key, value, y, base, prior, local, ridge, later, later_local):
    shape = matrices_like(local)
    args = (query, key, value, y, base, prior, local, ridge, later, later_local)
    out = jax.ShapeDtypeStruct(key.shape, bf16)
    return call(first_kernel, core, args, [WHOLE] * 3, [out, shape, shape], "first_solve", 3 * 10**9)


def second_solve(core, query, key, value, y, base, prior, local, done):
    args = (query, key, value, y, base, prior, local, done)
    out = jax.ShapeDtypeStruct(query.shape, bf16)
    units = query.shape[0] // CHUNK * (key.shape[1] // (2 * DH))
    scratch = [pltpu.VMEM(key.shape, bf16), pltpu.SemaphoreType.DMA((units + 1,))]
    spec = pl.BlockSpec(memory_space=pltpu.HBM)
    return call(second_kernel, core, args, spec, out, "second_solve", 3 * 10**9, scratch)


def exchange(x):
    return lax.all_to_all(x, PLANE, 0, 0)


def swapped(x):
    return lax.ppermute(x, CORE, [(0, 1), (1, 0)])


def body(query_rows, key_rows, value_rows, key_gain, regularizer):
    place = lax.axis_index(CORE)
    core = place.astype(jnp.int32).reshape(1)
    chips = lax.axis_size(PLANE)
    core, is_first, is_second = lax.optimization_barrier((core, place == 0, place == 1))
    send, local1, scaled1, ridge1 = grams(1, core, key_gain, regularizer, key_rows, value_rows)
    received = swapped(send)
    keep, local0, scaled0, ridge0 = grams(0, core, key_gain, regularizer, key_rows, value_rows)
    pieces = exchange((keep + received).reshape(chips, 1, -1))
    before = exchange(sums_before(pieces)).reshape(keep.shape)
    mine = before + jnp.where(is_second, received, 0.0)
    other = swapped(before + jnp.where(is_first, keep, 0.0))
    base, y = preconditioners(core, ridge0, mine, local0)
    done, base1, y1 = first_solve(
        core, query_rows, scaled0, value_rows, y, base, mine, local0, ridge1, other, local1
    )
    return second_solve(core, query_rows, scaled1, value_rows, y1, base1, other, local1, done)


def solution(mesh):
    torus = Mesh(
        mesh.devices.reshape(8, 4, 2, mesh.shape["head"]), ("seq_0", "seq_1", "seq_2", "head")
    )
    in_specs = (P(SEQ, "head"), P(SEQ, "head"), P(SEQ, "head"), P("head"), P("head"))
    out_specs = P(SEQ, "head")
    return jax.shard_map(body, mesh=torus, in_specs=in_specs, out_specs=out_specs, check_vma=False)
```

```python
import functools
import jax
import jax.numpy as jnp
from jax import lax
from jax.experimental import pallas as pl
from jax.experimental.pallas import tpu as pltpu
from jax.sharding import Mesh
from jax.sharding import PartitionSpec as P

DH = 128
NS_STEPS = 8
REFINE = 2
CHUNK = 256
VMEM = 20 * 2**20
PAIR = 400
SEQ = ("seq_0", "seq_1", "seq_2")
PLANE = ("seq_1", "seq_0")
CORE = "seq_2"

f32 = jnp.float32
bf16 = jnp.bfloat16


def mm(left, right):
    return jnp.dot(left, right, preferred_element_type=f32)


def mm_tn(left, right):
    return lax.dot_general(left, right, (((0,), (0,)), ((), ())), preferred_element_type=f32)


def mm_nt(left, right):
    return lax.dot_general(left, right, (((1,), (1,)), ((), ())), preferred_element_type=f32)


def split(x):
    high = x.astype(bf16)
    return high, (x - high.astype(f32)).astype(bf16)


def side(x):
    return jnp.concatenate(split(x), axis=1)


def doubled(x):
    x = side(x)
    return jnp.concatenate([x, x], axis=0)


def fold(x):
    return x[:, :DH] + x[:, DH:]


def eye():
    rows = lax.broadcasted_iota(jnp.int32, (DH, DH), 0)
    columns = lax.broadcasted_iota(jnp.int32, (DH, DH), 1)
    return (rows == columns).astype(f32)


def scaled_keys(key, gain):
    return (key.astype(f32) * gain).astype(bf16)


def in_hbm(*arrays):
    return [pltpu.with_memory_space_constraint(x, pltpu.HBM) for x in arrays]


def triangles():
    rows = lax.broadcasted_iota(jnp.int32, (DH, DH), 0)
    columns = lax.broadcasted_iota(jnp.int32, (DH, DH), 1)
    return rows <= columns, rows == columns


def gram_kernel(which, core_ref, gain_ref, reg_ref, k_ref, v_ref, slab_ref, local_ref, scaled_ref, ridge_ref):
    half = 1 - core_ref[0] if which else core_ref[0]
    both = []
    for a in range(2):
        h = 2 * (half * pl.num_programs(0) + pl.program_id(0)) + a
        columns = slice(a * DH, (a + 1) * DH)
        k = scaled_keys(k_ref[:, columns], gain_ref[h])
        scaled_ref[:, columns] = k
        ridge_ref[a] = jnp.full(ridge_ref.shape[1:], reg_ref[h])
        pair = jnp.concatenate([k, v_ref[:, columns]], axis=1)
        first = mm_tn(k[:CHUNK], pair[:CHUNK])
        local_ref[a, 0] = first[:, :DH]
        local_ref[a, 1] = first[:, DH:]
        both.append(first + mm_tn(k[CHUNK:], pair[CHUNK:]))
        local_ref[a, 2] = both[a][:, :DH]
    one, two = both[0][:, :DH], both[1][:, :DH]
    above, on = triangles()
    for a in range(2):
        slab_ref[0, a * DH : (a + 1) * DH] = both[a][:, DH:]
    slab_ref[0, 2 * DH : 3 * DH] = jnp.where(above, one, two)
    diagonal = jnp.sum(jnp.where(on, two, 0.0), axis=0, keepdims=True)
    slab_ref[0, 3 * DH :] = jnp.broadcast_to(diagonal, (PAIR - 3 * DH, DH))


def grams(which, core, gain, reg, key, value):
    gain, reg, key, value = in_hbm(gain, reg, key, value)
    rows, width = key.shape
    steps = width // DH // 4
    smem = pl.BlockSpec(memory_space=pltpu.SMEM)
    wide = pl.BlockSpec((rows, 2 * DH), lambda i, c: (0, i + steps * (1 - c[0] if which else c[0])))
    return pl.pallas_call(
        functools.partial(gram_kernel, which),
        grid_spec=pltpu.PrefetchScalarGridSpec(
            num_scalar_prefetch=1,
            grid=(steps,),
            in_specs=[smem, smem, wide, wide],
            out_specs=[
                pl.BlockSpec((1, PAIR, DH), lambda i, c: (i, 0, 0)),
                pl.BlockSpec((2, 3, DH, DH), lambda i, c: (i, 0, 0, 0)),
                pl.BlockSpec((rows, 2 * DH), lambda i, c: (0, i)),
                pl.BlockSpec((2, 8, DH), lambda i, c: (i, 0, 0)),
            ],
        ),
        out_shape=[
            jax.ShapeDtypeStruct((steps, PAIR, DH), f32),
            jax.ShapeDtypeStruct((2 * steps, 3, DH, DH), f32),
            jax.ShapeDtypeStruct((rows, width // 2), bf16),
            jax.ShapeDtypeStruct((2 * steps, 8, DH), f32),
        ],
        compiler_params=pltpu.CompilerParams(vmem_limit_bytes=VMEM),
        cost_estimate=pl.CostEstimate(flops=10**9, bytes_accessed=2 * 10**6, transcendentals=0),
        name=f"grams_{which}",
    )(core, gain, reg, key, value)


def running_kernel(row, x_ref, o_ref):
    line = x_ref.shape[0] // row
    order = [y * line + z for z in range(line) for y in range(row)]
    total = x_ref[0]
    o_ref[0] = jnp.zeros_like(total)
    for j in order[1:]:
        o_ref[j] = total
        if j != order[-1]:
            total = total + x_ref[j]


def sums_before(pieces):
    return pl.pallas_call(
        functools.partial(running_kernel, lax.axis_size(PLANE[0])),
        out_shape=jax.ShapeDtypeStruct(pieces.shape, f32),
        in_specs=[pl.BlockSpec(memory_space=pltpu.VMEM)],
        out_specs=pl.BlockSpec(memory_space=pltpu.VMEM),
        compiler_params=pltpu.CompilerParams(vmem_limit_bytes=VMEM),
        name="sums_before",
    )(pieces)


def newton_schulz(ridge_ref, prior_ref, local_ref, base_ref, y_ref):
    heads = range(local_ref.shape[0])
    inverse, approx, product = {}, {}, {}

    def begin():
        identity = eye()
        above, on = triangles()
        priors = []
        for pair in range(prior_ref.shape[0]):
            packed = prior_ref[pair, 2 * DH : 3 * DH]
            turned = packed.T
            diagonal = prior_ref[pair, 3 * DH : 3 * DH + 1]
            priors.append(jnp.where(above, packed, turned))
            priors.append(jnp.where(on, diagonal, jnp.where(above, turned, packed)))
        for i in heads:
            base = identity * ridge_ref[i, :1] + priors[i]
            base_ref[i] = base
            end = base + local_ref[i, 2]
            squares = jnp.sum(jnp.sum(end * end, axis=0, keepdims=True), axis=1, keepdims=True)
            inverse[i] = 1.0 / jnp.sqrt(squares)
            z = end * inverse[i]
            approx[i] = 2.0 * identity - z
            product[i] = 2.0 * z - fold(mm(side(z), doubled(z)))

    def step():
        for i in heads:
            rows = side(product[i])
            weights = jnp.concatenate([rows, rows], axis=0)
            both = fold(mm(jnp.concatenate([rows, side(approx[i])], axis=0), weights))
            product[i], approx[i] = 2.0 * product[i] - both[:DH], 2.0 * approx[i] - both[DH:]

    def end():
        for i in heads:
            last = 2.0 * approx[i] - fold(mm(side(approx[i]), doubled(product[i])))
            y_ref[i] = last * inverse[i]

    return [begin] + [step] * (NS_STEPS - 2) + [end]


def diagonal_blocks(two):
    zero = jnp.zeros((DH, DH), two.dtype)
    upper = jnp.concatenate([two[:, :DH], zero], axis=1)
    lower = jnp.concatenate([zero, two[:, DH:]], axis=1)
    return jnp.concatenate([upper, lower], axis=0)


def halves_of(x):
    return x[:, :DH], x[:, DH:]


def beside(parts):
    high, low = (halves_of(x) for x in parts)
    return [jnp.concatenate([high[a], low[a]], axis=1) for a in range(2)]


def solving(half, q_ref, k_ref, v_ref, y_ref, base_ref, prior_ref, local_ref, o_ref, written=None):
    rows_in = q_ref.shape[0]
    width = q_ref.shape[1] // 2
    groups, weights = [], {}

    def begin():
        shape = (CHUNK, 2 * DH)
        columns = lax.rem(lax.broadcasted_iota(jnp.int32, shape, 1), DH)
        weights["causal"] = lax.broadcasted_iota(jnp.int32, shape, 0) >= columns
        for p in range(width // (2 * DH)):
            inside = slice(2 * p * DH, 2 * (p + 1) * DH)
            columns = pl.ds(pl.multiple_of(half * width + 2 * p * DH, 2 * DH), 2 * DH)
            group = []
            for a in range(2):
                y = side(y_ref[2 * p + a])
                weights[p, a] = y, jnp.concatenate([y, y], axis=0)
            for j in range(rows_in // CHUNK):
                rows = slice(j * CHUNK, (j + 1) * CHUNK)
                k, v = k_ref[rows, inside], v_ref[rows, columns]
                base, prior = [], []
                for a in range(2):
                    h = 2 * p + a
                    b, c = base_ref[h], prior_ref[p, a * DH : (a + 1) * DH]
                    base.append(doubled(b + local_ref[h, 0] if j else b))
                    prior.append(doubled(c + local_ref[h, 1] if j else c))
                blocks = lambda x: [diagonal_blocks(x[i * DH : (i + 1) * DH]) for i in range(CHUNK // DH)]
                group.append(dict(at=(rows, inside), q=q_ref[rows, columns], k=blocks(k), v=blocks(v), base=base, prior=prior))
            groups.append(group)
        through("s", 0, lambda c: halves_of(c["q"]))

    def through(key, which, rows_of):
        for p, group in enumerate(groups):
            parts = [rows_of(c) for c in group]
            out = []
            for a in range(2):
                rows = jnp.concatenate([x[a] for x in parts], axis=0)
                out.append(fold(mm(rows, weights[p, a][which])))
            for n, c in enumerate(group):
                c[key] = jnp.concatenate([x[n * CHUNK : (n + 1) * CHUNK] for x in out], axis=1)

    def each(function):
        def run():
            for group in groups:
                for c in group:
                    function(c)

        return run

    def score(c):
        c["parts"] = split(c["s"])
        high = c["parts"][0]
        c["scores"] = []
        for i, k in enumerate(c["k"]):
            scores = mm_nt(high[i * DH :], k)
            causal = weights["causal"][: CHUNK - i * DH]
            c["scores"].append(jnp.where(causal, scores, 0.0).astype(bf16))

    def times(c, matrices):
        rows = beside(c["parts"])
        return jnp.concatenate([fold(mm(rows[a], matrices[a])) for a in range(2)], axis=1)

    def causal_sum(c, values):
        first = mm(c["scores"][0], values[0])
        return jnp.concatenate([first[:DH], first[DH:] + mm(c["scores"][1], values[1])], axis=0)

    def residual(c):
        c["residual"] = c["q"].astype(f32) - times(c, c["base"]) - causal_sum(c, c["k"])

    def correct():
        through("step", 1, lambda c: beside(split(c["residual"])))
        for group in groups:
            for c in group:
                c["s"] = c["s"] + c["step"]

    def readout(c):
        o_ref[c["at"]] = (times(c, c["prior"]) + causal_sum(c, c["v"])).astype(bf16)
        if written is not None:
            written(c["at"])

    return [begin] + [each(score), each(residual), correct] * REFINE + [each(score), each(readout)]


def precond_kernel(ridge_ref, prior_ref, local_ref, base_ref, y_ref):
    for step in newton_schulz(ridge_ref, prior_ref, local_ref, base_ref, y_ref):
        step()


def first_kernel(
    core_ref, q_ref, k_ref, v_ref, y_ref, base_ref, prior_ref, local_ref,
    ridge_ref, later_prior_ref, later_local_ref, o_ref, later_base_ref, later_y_ref,
):
    mine = solving(core_ref[0], q_ref, k_ref, v_ref, y_ref, base_ref, prior_ref, local_ref, o_ref)
    later = newton_schulz(ridge_ref, later_prior_ref, later_local_ref, later_base_ref, later_y_ref)
    for i, step in enumerate(mine):
        step()
        if i:
            later[i - 1]()


def second_kernel(
    core_ref, q_ref, k_ref, v_ref, y_ref, base_ref, prior_ref, local_ref, done_ref, o_ref, out_ref, sems
):
    width = done_ref.shape[1]
    half = 1 - core_ref[0]
    copies = []

    def send(source, rows, start, size, number):
        columns = pl.ds(pl.multiple_of(start, 2 * DH), size)
        copies.append(pltpu.make_async_copy(source, o_ref.at[rows, columns], sems.at[number]))
        copies[-1].start()

    def written(at):
        rows, columns = at
        size = columns.stop - columns.start
        send(out_ref.at[rows, columns], rows, half * width + columns.start, size, len(copies))

    send(done_ref, slice(None), core_ref[0] * width, width, 0)
    for step in solving(half, q_ref, k_ref, v_ref, y_ref, base_ref, prior_ref, local_ref, out_ref, written):
        step()
    for copy in copies:
        copy.wait()


WHOLE = pl.BlockSpec(memory_space=pltpu.VMEM)


def call(kernel, core, args, out_specs, out_shape, name, flops, scratch=()):
    return pl.pallas_call(
        kernel,
        grid_spec=pltpu.PrefetchScalarGridSpec(
            num_scalar_prefetch=1, grid=(1,), in_specs=[WHOLE] * len(args), out_specs=out_specs,
            scratch_shapes=scratch,
        ),
        out_shape=out_shape,
        compiler_params=pltpu.CompilerParams(vmem_limit_bytes=VMEM),
        cost_estimate=pl.CostEstimate(flops=flops, bytes_accessed=2 * 10**6, transcendentals=0),
        name=name,
    )(core, *args)


def precond_first_kernel(core_ref, *refs):
    precond_kernel(*refs)


def matrices_like(local):
    return jax.ShapeDtypeStruct((local.shape[0], DH, DH), f32)


def preconditioners(core, ridge, prior, local):
    shape = matrices_like(local)
    args = (ridge, prior, local)
    return call(precond_first_kernel, core, args, [WHOLE] * 2, [shape] * 2, "preconditioners", 10**9)


def first_solve(core, query, key, value, y, base, prior, local, ridge, later, later_local):
    shape = matrices_like(local)
    args = (query, key, value, y, base, prior, local, ridge, later, later_local)
    out = jax.ShapeDtypeStruct(key.shape, bf16)
    return call(first_kernel, core, args, [WHOLE] * 3, [out, shape, shape], "first_solve", 3 * 10**9)


def second_solve(core, query, key, value, y, base, prior, local, done):
    args = (query, key, value, y, base, prior, local, done)
    out = jax.ShapeDtypeStruct(query.shape, bf16)
    units = query.shape[0] // CHUNK * (key.shape[1] // (2 * DH))
    scratch = [pltpu.VMEM(key.shape, bf16), pltpu.SemaphoreType.DMA((units + 1,))]
    spec = pl.BlockSpec(memory_space=pltpu.HBM)
    return call(second_kernel, core, args, spec, out, "second_solve", 3 * 10**9, scratch)


def exchange(x):
    return lax.all_to_all(x, PLANE, 0, 0)


def swapped(x):
    return lax.ppermute(x, CORE, [(0, 1), (1, 0)])


def body(query_rows, key_rows, value_rows, key_gain, regularizer):
    place = lax.axis_index(CORE)
    core = place.astype(jnp.int32).reshape(1)
    chips = lax.axis_size(PLANE)
    core, is_first, is_second = lax.optimization_barrier((core, place == 0, place == 1))
    send, local1, scaled1, ridge1 = grams(1, core, key_gain, regularizer, key_rows, value_rows)
    received = swapped(send)
    keep, local0, scaled0, ridge0 = grams(0, core, key_gain, regularizer, key_rows, value_rows)
    pieces = exchange((keep + received).reshape(chips, 1, -1))
    before = exchange(sums_before(pieces)).reshape(keep.shape)
    mine = before + jnp.where(is_second, received, 0.0)
    other = swapped(before + jnp.where(is_first, keep, 0.0))
    base, y = preconditioners(core, ridge0, mine, local0)
    done, base1, y1 = first_solve(
        core, query_rows, scaled0, value_rows, y, base, mine, local0, ridge1, other, local1
    )
    return second_solve(core, query_rows, scaled1, value_rows, y1, base1, other, local1, done)


def solution(mesh):
    torus = Mesh(
        mesh.devices.reshape(8, 4, 2, mesh.shape["head"]), ("seq_0", "seq_1", "seq_2", "head")
    )
    in_specs = (P(SEQ, "head"), P(SEQ, "head"), P(SEQ, "head"), P("head"), P("head"))
    out_specs = P(SEQ, "head")
    return jax.shard_map(body, mesh=torus, in_specs=in_specs, out_specs=out_specs, check_vma=False)
```
